512 devices in a mesh: patch: 128 (over y, z, core), rep: 4 (over x).
Axes of the slice: x: 4, y: 4, z: 16, core: 2. Of those that a mesh axis runs over, the one named last changes fastest.
Arguments:
- nodes: bfloat16 [4, 65536, 256], P('rep', 'patch'), may hold values from -6 to 6
- edges: bfloat16 [4, 196608, 256], P('rep', 'patch'), may hold values from -6 to 6
- edge_ends: int32 [196608, 2], P('patch'), may hold values from 0 to 543, as said below
- edge_count: int32 [128], P('patch'), may hold values from 768 to 1536, as said below
- send_rows: int32 [256, 16], P('patch'), may hold values from 0 to 511, as said below
- cotangent: bfloat16 [4, 65536, 256], P('rep', 'patch'), may hold values from -6 to 6
- edge_first: bfloat16 [768, 256], replicated, may hold values from -0.21875 to 0.21875
- edge_second: bfloat16 [256, 256], replicated, may hold values from -0.375 to 0.375
- node_first: bfloat16 [512, 256], replicated, may hold values from -0.25 to 0.25
- node_second: bfloat16 [256, 256], replicated, may hold values from -0.375 to 0.375
Outputs:
- new_nodes: bfloat16 [4, 65536, 256], P('rep', 'patch')
- grad_nodes: bfloat16 [4, 65536, 256], P('rep', 'patch')
- grad_edges: bfloat16 [4, 196608, 256], P('rep', 'patch')
- grad_edge_first: bfloat16 [768, 256], replicated
- grad_edge_second: bfloat16 [256, 256], replicated
- grad_node_first: bfloat16 [512, 256], replicated
- grad_node_second: bfloat16 [256, 256], replicated
The draws below stay inside these ranges and needn't reach their ends.
Inputs may be any that keep to these rules, and one draw needn't show every extreme that they name: `edge_ends`: in patch p's block, row j gives edge slot j: column 0 is a vertex of p; column 1 is a vertex of p, or 512 + h * 16 + s with h < 2, which names the vertex in slot s of row h of the send_rows block of patch (p + h + 1) mod 128. Padding slots hold ends of the same form. `edge_count`: live edge slots of each patch; slots at or beyond it are padding. Some patch has all 1536 live. `send_rows`: each patch's block has 2 rows of 16 distinct vertices of that patch, in its own numbering.
All inputs are finite; a program needn't handle non-finite values.
Results may differ from the reference program's by a relative error of at most 0.0084.
Values may be sent and summed in bfloat16 or wider, within the bound.
No kernel may reach another device: no remote copies, remote signals or barrier semaphores. Data moves between devices by JAX's collectives and lax.ppermute only.
A program may use at most 64 MiB of HBM per device.

```python
import jax
import jax.numpy as jnp
from jax import lax

D = 256
V_DEV = 512
HOPS = 2
EDGE_DEV = 1536
SLOT = 16
SNAPS = 4
VERTS = 65536
EDGES = 196608
N_PATCH = 128


def draw_edge_ends(key, part):
    first_key, cut_key, choose_key, other_key = jax.random.split(jax.random.fold_in(key, 11), 4)
    first_end = jax.random.randint(first_key, (EDGES,), 0, V_DEV, dtype=jnp.int32)
    is_cut = jax.random.randint(cut_key, (EDGES,), 0, 4 * EDGE_DEV, dtype=jnp.int32) < 5 * HOPS * SLOT
    remote = V_DEV + jax.random.randint(choose_key, (EDGES,), 0, HOPS * SLOT, dtype=jnp.int32)
    nearby = (first_end + 1 + jax.random.randint(other_key, (EDGES,), 0, V_DEV - 1, dtype=jnp.int32)) % V_DEV
    second_end = jnp.where(is_cut, remote, nearby)
    return jnp.stack([first_end, second_end], axis=1).astype(jnp.int32)


def draw_edge_count(key, part):
    count_key, top_key = jax.random.split(jax.random.fold_in(key, 12))
    patches = EDGES // EDGE_DEV
    counts = jax.random.randint(count_key, (patches,), EDGE_DEV // 2, EDGE_DEV + 1, dtype=jnp.int32)
    fullest = jax.random.randint(top_key, (), 0, patches, dtype=jnp.int32)
    return jnp.where(jnp.arange(patches, dtype=jnp.int32) == fullest, EDGE_DEV, counts).astype(jnp.int32)


def pick_rows(one_key):
    return jax.random.permutation(one_key, V_DEV)[:SLOT]


def draw_send_rows(key, part):
    keys = jax.random.split(jax.random.fold_in(key, 13), EDGES // EDGE_DEV * HOPS)
    return jax.vmap(pick_rows)(keys).astype(jnp.int32)


def shard_levels(stream_key, shape, pieces, low, high):
    def one(dim, blocks):
        steps = jax.random.uniform(jax.random.fold_in(jax.random.fold_in(stream_key, 6), dim), (blocks,), jnp.float32, low / len(pieces), high / len(pieces))
        return jnp.repeat(jnp.exp(steps), shape[dim] // blocks).reshape((-1,) + (1,) * (len(shape) - dim - 1))

    level = one(*pieces[0])
    for cut in pieces[1:]:
        level = level * one(*cut)
    return level


def normal_values(key, shape, scale, limit, cuts=(), kind=jnp.bfloat16):
    loudness = shard_levels(key, shape, cuts, -0.22, 0.18) if cuts else 1.0
    result = jax.random.normal(key, shape, jnp.float32) * scale * loudness
    return jnp.minimum(jnp.maximum(result, -limit), limit).astype(kind)


def setup_inputs(seed: int = 0) -> dict:
    key_list = jax.random.split(jax.random.key(seed), 11)
    return {
        "nodes": normal_values(key_list[0], (SNAPS, VERTS, D), 1.0, 6.0, ((0, 4), (1, 128))),
        "edges": normal_values(key_list[1], (SNAPS, EDGES, D), 1.0, 6.0, ((0, 4), (1, 128))),
        "edge_ends": draw_edge_ends(jax.random.fold_in(key_list[10], 71), 0),
        "edge_count": draw_edge_count(jax.random.fold_in(key_list[10], 71), 0),
        "send_rows": draw_send_rows(jax.random.fold_in(key_list[10], 71), 0),
        "cotangent": normal_values(key_list[5], (SNAPS, VERTS, D), 1.0, 6.0, ((0, 4), (1, 128))),
        "edge_first": normal_values(key_list[6], (3 * D, D), (3 * D) ** -0.5, 0.21875),
        "edge_second": normal_values(key_list[7], (D, D), D ** -0.5, 0.375),
        "node_first": normal_values(key_list[8], (2 * D, D), (2 * D) ** -0.5, 0.25),
        "node_second": normal_values(key_list[9], (D, D), D ** -0.5, 0.375),
    }


EPS = 1e-05

def normalize(values):
    average = lax.optimization_barrier(jnp.mean(values, axis=-1, keepdims=True))
    centred = values - average
    inv_scale = lax.rsqrt(lax.optimization_barrier(jnp.mean(centred * centred, axis=-1, keepdims=True)) + EPS)
    return (centred * inv_scale, inv_scale)

def norm_back(upstream, normed, inv_scale):
    return inv_scale * (upstream - lax.optimization_barrier(jnp.mean(upstream, axis=-1, keepdims=True)) - normed * lax.optimization_barrier(jnp.mean(upstream * normed, axis=-1, keepdims=True)))

def silu_slope(pre):
    sigma = jax.nn.sigmoid(pre)
    return sigma * (1.0 + pre * (1.0 - sigma))

def matmul(left, right):
    return jnp.dot(left, right, preferred_element_type=jnp.float32)

def outer_sum(left, right):
    return lax.dot_general(left, right, (((0,), (0,)), ((), ())), preferred_element_type=jnp.float32)

def global_ends(edge_ends, edge_count, send_rows):
    owner = jnp.arange(EDGES, dtype=jnp.int32) // EDGE_DEV
    first_end = (owner * V_DEV + edge_ends[:, 0]).astype(jnp.int32)
    second = edge_ends[:, 1].astype(jnp.int32)
    remote = second - V_DEV
    offset = jnp.clip(remote // SLOT, 0, HOPS - 1).astype(jnp.int32)
    position = (remote % SLOT).astype(jnp.int32)
    partner = ((owner + offset + 1) % N_PATCH).astype(jnp.int32)
    far_row = partner * V_DEV + send_rows[partner * HOPS + offset, position]
    second_end = jnp.where(second < V_DEV, owner * V_DEV + second, far_row).astype(jnp.int32)
    slot_index = jnp.arange(EDGES, dtype=jnp.int32) % EDGE_DEV
    alive = (slot_index < edge_count[owner]).astype(jnp.float32)[:, None]
    return (first_end, second_end, alive)

def snapshot(node_rows, edge_rows, cot_rows, first_end, second_end, alive, edge_first, edge_second, node_first, node_second):
    features = node_rows.shape[1]
    first_rows = node_rows[first_end]
    second_rows = node_rows[second_end]
    edge_pre = matmul(edge_rows, edge_first[:features]) + matmul(first_rows, edge_first[features:2 * features]) + matmul(second_rows, edge_first[2 * features:])
    edge_hidden = jax.nn.silu(edge_pre).astype(jnp.bfloat16)
    edge_normed, edge_inv = normalize(matmul(edge_hidden, edge_second))
    new_edge = ((edge_rows.astype(jnp.float32) + edge_normed) * alive).astype(jnp.bfloat16)
    new_wide = lax.optimization_barrier(new_edge).astype(jnp.float32)
    verts = node_rows.shape[0]
    aggregate = (jax.ops.segment_sum(new_wide, first_end, verts) + jax.ops.segment_sum(new_wide, second_end, verts)).astype(jnp.bfloat16)
    node_pre = matmul(node_rows, node_first[:features]) + matmul(aggregate, node_first[features:])
    node_hidden = jax.nn.silu(node_pre).astype(jnp.bfloat16)
    node_normed, node_inv = normalize(matmul(node_hidden, node_second))
    new_nodes = (node_rows.astype(jnp.float32) + node_normed).astype(jnp.bfloat16)
    cot_wide = cot_rows.astype(jnp.float32)
    d_node_out = norm_back(cot_wide, node_normed, node_inv).astype(jnp.bfloat16)
    grad_ns = outer_sum(node_hidden, d_node_out)
    d_node_pre = (matmul(d_node_out, node_second.T) * silu_slope(node_pre)).astype(jnp.bfloat16)
    grad_nf = jnp.concatenate([outer_sum(node_rows, d_node_pre), outer_sum(aggregate, d_node_pre)], axis=0)
    d_direct = matmul(d_node_pre, node_first[:features].T)
    d_aggregate = matmul(d_node_pre, node_first[features:].T).astype(jnp.bfloat16)
    d_new_edge = alive * (d_aggregate[first_end].astype(jnp.float32) + d_aggregate[second_end].astype(jnp.float32))
    d_edge_out = norm_back(d_new_edge, edge_normed, edge_inv).astype(jnp.bfloat16)
    grad_es = outer_sum(edge_hidden, d_edge_out)
    d_edge_pre = (matmul(d_edge_out, edge_second.T) * silu_slope(edge_pre)).astype(jnp.bfloat16)
    grad_ef = jnp.concatenate([outer_sum(edge_rows, d_edge_pre), outer_sum(first_rows, d_edge_pre), outer_sum(second_rows, d_edge_pre)], axis=0)
    grad_edges = (d_new_edge + matmul(d_edge_pre, edge_first[:features].T)).astype(jnp.bfloat16)
    d_first_end = matmul(d_edge_pre, edge_first[features:2 * features].T)
    d_second_end = matmul(d_edge_pre, edge_first[2 * features:].T)
    grad_nodes = (cot_wide + d_direct + jax.ops.segment_sum(d_first_end, first_end, verts) + jax.ops.segment_sum(d_second_end, second_end, verts)).astype(jnp.bfloat16)
    return (new_nodes, grad_nodes, grad_edges, grad_ef, grad_es, grad_nf, grad_ns)

def reference(nodes, edges, edge_ends, edge_count, send_rows, cotangent, edge_first, edge_second, node_first, node_second):
    first_end, second_end, alive = global_ends(edge_ends, edge_count, send_rows)

    def one_snapshot(inputs):
        return snapshot(inputs[0], inputs[1], inputs[2], first_end, second_end, alive, edge_first, edge_second, node_first, node_second)
    results = lax.map(one_snapshot, (nodes, edges, cotangent))
    new_nodes, grad_nodes, grad_edges = (results[0], results[1], results[2])
    summed = [lax.optimization_barrier(jnp.sum(part, axis=0)).astype(jnp.bfloat16) for part in results[3:]]
    return (new_nodes, grad_nodes, grad_edges, summed[0], summed[1], summed[2], summed[3])
```

```python
import jax
import jax.numpy as jnp
from jax import lax
from jax.experimental import pallas as pl
from jax.experimental.pallas import tpu as pltpu
from jax.sharding import Mesh, PartitionSpec as P

EPS = 1e-05
BF = jnp.bfloat16
F32 = jnp.float32
BLOCK = 512
PATCH_SPLIT = (4, 8, 2, 2)
PATCH = ("y", "zh", "zl", "c")
INNER = ("y", "zl", "c", "rep")
OUTER = ("zh",)


def dot(left, right):
    return jnp.dot(left, right, preferred_element_type=F32)


def dot_t(left, right):
    return lax.dot_general(left, right, (((1,), (1,)), ((), ())), preferred_element_type=F32)


def t_dot(left, right):
    return lax.dot_general(left, right, (((0,), (0,)), ((), ())), preferred_element_type=F32)


def split(values):
    high = values.astype(BF)
    return high, (values - high.astype(F32)).astype(BF)


def one_hot(index, shape, axis):
    return (index == lax.broadcasted_iota(jnp.int32, shape, axis)).astype(F32)


def normalize(values):
    centred = values - jnp.mean(values, axis=-1, keepdims=True)
    inv_scale = lax.rsqrt(jnp.mean(centred * centred, axis=-1, keepdims=True) + EPS)
    return centred * inv_scale, inv_scale


def norm_back(upstream, normed, inv_scale):
    return inv_scale * (
        upstream
        - jnp.mean(upstream, axis=-1, keepdims=True)
        - normed * jnp.mean(upstream * normed, axis=-1, keepdims=True)
    )


def sigmoid(pre):
    return 1.0 / (1.0 + jnp.exp(-pre))


def slope(pre):
    sigma = sigmoid(pre)
    return sigma * (1.0 + pre * (1.0 - sigma))


def live_row(ends_ref, row, start, count, offset=0):
    index = ends_ref[row : row + 1, pl.ds(start, BLOCK)]
    slot = start + lax.broadcasted_iota(jnp.int32, (1, BLOCK), 1)
    return jnp.where(slot < count, index - offset, -1)


def loop(total, body):
    def step(i, carry):
        body(pl.multiple_of(i * BLOCK, BLOCK))
        return carry

    lax.fori_loop(0, total // BLOCK, step, 0)


def seam_pick(send_ref, hop, table):
    verts = table.shape[0]
    slots = send_ref.shape[1]
    pick = one_hot(send_ref[hop : hop + 1, :], (verts, slots), 0).astype(BF)
    return t_dot(pick, table).astype(BF)


def seam_spread(send_ref, hop, verts, rows):
    slots = send_ref.shape[1]
    pick = one_hot(send_ref[hop : hop + 1, :], (verts, slots), 0)
    return jnp.dot(pick, rows, preferred_element_type=F32, precision=lax.Precision.HIGHEST)


def seam_kernel(send_ref, nodes_ref, out0_ref, out1_ref):
    table = nodes_ref[...]
    out0_ref[...] = seam_pick(send_ref, 0, table)
    out1_ref[...] = seam_pick(send_ref, 1, table)


def edge_local_kernel(
    count_ref, ends_ref, nodes_ref, edges_ref, ef_ref, pre_ref, pairs_ref, far_ref
):
    features = nodes_ref.shape[1]
    verts = nodes_ref.shape[0]
    seam = far_ref.shape[1]
    count = count_ref[0]

    def body(start):
        rows = pl.ds(start, BLOCK)
        first = live_row(ends_ref, 0, start, count)
        second = live_row(ends_ref, 1, start, count)
        both = jnp.concatenate([first, second, second, second, second, second, second, second], axis=0)
        cols = both.T
        first_col = cols[:, 0:1]
        second_col = cols[:, 1:2]
        pick_first = one_hot(first_col, (BLOCK, verts), 1)
        pick_second = one_hot(second_col, (BLOCK, verts), 1)
        far_ref[rows, :] = one_hot(second_col - verts, (BLOCK, seam), 1).astype(BF)
        pairs_ref[rows, :] = (pick_first + pick_second).astype(BF)
        table = nodes_ref[...]
        first_rows = dot(pick_first.astype(BF), table).astype(BF)
        second_rows = dot(pick_second.astype(BF), table).astype(BF)
        pre_ref[rows, :] = (
            dot(edges_ref[rows, :], ef_ref[:features, :])
            + dot(first_rows, ef_ref[features : 2 * features, :])
            + dot(second_rows, ef_ref[2 * features :, :])
        )

    loop(edges_ref.shape[0], body)


def edge_forward_kernel(
    count_ref,
    ends_ref,
    halo0_ref,
    halo1_ref,
    edges_ref,
    part_ref,
    far_ref,
    ef_ref,
    es_ref,
    pre_ref,
    hidden_ref,
    normed_ref,
    inv_ref,
    agg_ref,
    back0_ref,
    back1_ref,
    seam_ref,
):
    features = edges_ref.shape[1]
    verts = agg_ref.shape[0]
    slots = halo0_ref.shape[0]
    count = count_ref[0]
    halo = jnp.concatenate([halo0_ref[...], halo1_ref[...]], axis=0)
    agg_ref[...] = jnp.zeros_like(agg_ref)
    seam_ref[...] = jnp.zeros_like(seam_ref)

    def body(start):
        rows = pl.ds(start, BLOCK)
        far_rows = dot(far_ref[rows, :], halo).astype(BF)
        pre = part_ref[rows, :] + dot(far_rows, ef_ref[2 * features :, :])
        pre_ref[rows, :] = pre
        hidden = (pre * sigmoid(pre)).astype(BF)
        hidden_ref[rows, :] = hidden
        normed, inv = normalize(dot(hidden, es_ref[...]))
        normed_ref[rows, :] = normed
        inv_ref[rows, :] = inv
        new_edge = (edges_ref[rows, :].astype(F32) + normed).astype(BF)
        first = live_row(ends_ref, 0, start, count)
        second = live_row(ends_ref, 1, start, count)
        spread = one_hot(first, (verts, BLOCK), 0) + one_hot(second, (verts, BLOCK), 0)
        agg_ref[...] += dot(spread.astype(BF), new_edge)
        away = one_hot(second - verts, (2 * slots, BLOCK), 0).astype(BF)
        seam_ref[...] += dot(away, new_edge)

    loop(edges_ref.shape[0], body)
    back0_ref[...] = seam_ref[:slots, :]
    back1_ref[...] = seam_ref[slots:, :]


def node_kernel(
    send_ref,
    nodes_ref,
    cot_ref,
    agg_ref,
    got0_ref,
    got1_ref,
    nf_ref,
    ns_ref,
    new_ref,
    agg16_ref,
    hidden_ref,
    dout_ref,
    dpre_ref,
    dagg_ref,
    out0_ref,
    out1_ref,
):
    verts, features = nodes_ref.shape
    total = agg_ref[...] + seam_spread(send_ref, 0, verts, got0_ref[...])
    total = total + seam_spread(send_ref, 1, verts, got1_ref[...])
    aggregate = total.astype(BF)
    agg16_ref[...] = aggregate
    node_rows = nodes_ref[...]
    pre = dot(node_rows, nf_ref[:features, :]) + dot(aggregate, nf_ref[features:, :])
    sigma = sigmoid(pre)
    hidden = (pre * sigma).astype(BF)
    hidden_ref[...] = hidden
    normed, inv = normalize(dot(hidden, ns_ref[...]))
    new_ref[...] = (node_rows.astype(F32) + normed).astype(BF)
    d_out = norm_back(cot_ref[...].astype(F32), normed, inv).astype(BF)
    dout_ref[...] = d_out
    d_pre = (dot_t(d_out, ns_ref[...]) * (sigma * (1.0 + pre * (1.0 - sigma)))).astype(BF)
    dpre_ref[...] = d_pre
    d_agg = dot_t(d_pre, nf_ref[features:, :]).astype(BF)
    dagg_ref[...] = d_agg
    out0_ref[...] = seam_pick(send_ref, 0, d_agg)
    out1_ref[...] = seam_pick(send_ref, 1, d_agg)


def fill_kernel(
    nodes_ref,
    cot_ref,
    agg16_ref,
    hidden_ref,
    dout_ref,
    dpre_ref,
    dagg_ref,
    nf_ref,
    pairs_ref,
    grad_ref,
    part_ref,
    up_ref,
):
    features = nodes_ref.shape[1]
    d_pre = dpre_ref[...]

    def body(start):
        rows = pl.ds(start, BLOCK)
        up_ref[rows, :] = dot(pairs_ref[rows, :], dagg_ref[...])

    loop(pairs_ref.shape[0], body)
    grad_ref[:features, :] = t_dot(nodes_ref[...], d_pre).astype(BF)
    grad_ref[features : 2 * features, :] = t_dot(agg16_ref[...], d_pre).astype(BF)
    grad_ref[2 * features :, :] = t_dot(hidden_ref[...], dout_ref[...]).astype(BF)
    part_ref[...] = cot_ref[...].astype(F32) + dot_t(d_pre, nf_ref[:features, :])


def edge_backward_kernel(
    count_ref,
    ends_ref,
    nodes_ref,
    halo0_ref,
    halo1_ref,
    edges_ref,
    up_ref,
    far_ref,
    dhalo0_ref,
    dhalo1_ref,
    pre_ref,
    hidden_ref,
    normed_ref,
    inv_ref,
    ef_ref,
    es_ref,
    nodegrad_ref,
    part_ref,
    gedges_ref,
    pack_ref,
    partout_ref,
    back0_ref,
    back1_ref,
    first_ref,
    second_ref,
    seam_ref,
    ges_ref,
    ge1_ref,
):
    features = edges_ref.shape[1]
    half = features // 2
    verts = nodes_ref.shape[0]
    slots = halo0_ref.shape[0]
    count = count_ref[0]
    d_halo = jnp.concatenate([dhalo0_ref[...], dhalo1_ref[...]], axis=0)
    for ref in (first_ref, second_ref, seam_ref, ges_ref, ge1_ref):
        ref[...] = jnp.zeros_like(ref)

    def body(start):
        rows = pl.ds(start, BLOCK)
        up = up_ref[rows, :] + dot(far_ref[rows, :], d_halo)
        d_out = norm_back(up, normed_ref[rows, :], inv_ref[rows, :]).astype(BF)
        ges_ref[...] += t_dot(hidden_ref[rows, :], d_out)
        d_pre = (dot_t(d_out, es_ref[...]) * slope(pre_ref[rows, :])).astype(BF)
        first = live_row(ends_ref, 0, start, count)
        second = live_row(ends_ref, 1, start, count)
        seam_ref[...] += dot(one_hot(second - verts, (2 * slots, BLOCK), 0).astype(BF), d_pre)
        first_ref[...] += dot(one_hot(first, (verts, BLOCK), 0).astype(BF), d_pre)
        second_ref[...] += dot(one_hot(second, (verts, BLOCK), 0).astype(BF), d_pre)
        ge1_ref[...] += t_dot(edges_ref[rows, :], d_pre)
        gedges_ref[rows, :] = (up + dot_t(d_pre, ef_ref[:features, :])).astype(BF)

    loop(edges_ref.shape[0], body)
    back0_ref[...] = seam_ref[:slots, :]
    back1_ref[...] = seam_ref[slots:, :]
    total = pack_ref.shape[0] // 2

    def put(begin, grad):
        grad = grad.astype(BF)
        size = grad.shape[0]
        pack_ref[begin : begin + size, :] = grad[:, :half]
        pack_ref[total + begin : total + begin + size, :] = grad[:, half:]

    node_rows = nodes_ref[...]
    first_high, first_low = split(first_ref[...])
    second_high, second_low = split(second_ref[...])
    far_high, far_low = split(seam_ref[...])
    halo = jnp.concatenate([halo0_ref[...], halo1_ref[...]], axis=0)
    put(0, ge1_ref[...])
    put(features, t_dot(node_rows, first_high) + t_dot(node_rows, first_low))
    put(
        2 * features,
        t_dot(node_rows, second_high)
        + t_dot(node_rows, second_low)
        + t_dot(halo, far_high)
        + t_dot(halo, far_low),
    )
    put(3 * features, ges_ref[...])
    put(4 * features, nodegrad_ref[...])
    middle = ef_ref[features : 2 * features, :]
    last = ef_ref[2 * features :, :]
    partout_ref[...] = (
        part_ref[...]
        + (dot_t(first_high, middle) + dot_t(first_low, middle))
        + (dot_t(second_high, last) + dot_t(second_low, last))
    )


def finish_kernel(send_ref, part_ref, got0_ref, got1_ref, ef_ref, out_ref):
    verts, features = part_ref.shape
    last = ef_ref[2 * features :, :]
    total = part_ref[...]
    for hop, ref in enumerate((got0_ref, got1_ref)):
        high, low = split(ref[...])
        total = total + seam_spread(send_ref, hop, verts, dot_t(high, last) + dot_t(low, last))
    out_ref[...] = total.astype(BF)


def unpack_kernel(pack_ref, gef_ref, ges_ref, gnf_ref, gns_ref):
    total = pack_ref.shape[0] // 2
    half = pack_ref.shape[1]
    begin = 0
    for ref in (gef_ref, ges_ref, gnf_ref, gns_ref):
        size = ref.shape[0]
        ref[:, :half] = pack_ref[begin : begin + size, :]
        ref[:, half:] = pack_ref[total + begin : total + begin + size, :]
        begin += size


def call(kernel, outs, args, scalars=0, scratch=(), flops=0, name=None):
    return pl.pallas_call(
        kernel,
        out_shape=[jax.ShapeDtypeStruct(shape, kind) for shape, kind in outs],
        in_specs=[
            pl.BlockSpec(memory_space=pltpu.SMEM if i < scalars else pltpu.VMEM)
            for i in range(len(args))
        ],
        out_specs=[pl.BlockSpec(memory_space=pltpu.VMEM) for _ in outs],
        scratch_shapes=[pltpu.VMEM(shape, F32) for shape in scratch],
        cost_estimate=pl.CostEstimate(flops=flops, transcendentals=0, bytes_accessed=flops // 1000),
        name=name,
    )(*args)


def shift(block, distance):
    count = lax.axis_size(PATCH)
    return lax.ppermute(block, PATCH, [((i - distance) % count, i) for i in range(count)])


def group_size(axes):
    return lax.axis_size(axes)


def sum_everywhere(pack):
    inner = group_size(INNER)
    outer = group_size(OUTER)
    rows, lanes = pack.shape
    pieces = lax.all_to_all(pack.reshape(inner, rows // inner, lanes), INNER, 0, 0)
    mine = jnp.sum(pieces.astype(F32), axis=0).astype(BF)
    spread = jnp.broadcast_to(mine[None], (outer,) + mine.shape)
    pieces = lax.all_to_all(spread, OUTER, 0, 0)
    mine = jnp.sum(pieces.astype(F32), axis=0).astype(BF)
    spread = jnp.broadcast_to(mine[None], (inner,) + mine.shape)
    return lax.all_to_all(spread, INNER, 0, 0).reshape(rows, lanes)


def local(
    nodes,
    edges,
    edge_ends,
    edge_count,
    send_rows,
    cotangent,
    edge_first,
    edge_second,
    node_first,
    node_second,
):
    node_rows = nodes[0]
    edge_rows = edges[0]
    cot = cotangent[0]
    verts, features = node_rows.shape
    slots = edge_rows.shape[0]
    hops, seam = send_rows.shape
    assert hops == 2
    ends = edge_ends.T
    seam16 = ((seam, features), BF)
    seam32 = ((seam, features), F32)
    unit = 2 * features * features

    out0, out1 = call(seam_kernel, [seam16, seam16], (send_rows, node_rows), flops=10**8, name="seam")
    halo0 = shift(out0, -1)
    halo1 = shift(out1, -2)
    part, pairs, far = call(
        edge_local_kernel,
        [((slots, features), F32), ((slots, verts), BF), ((slots, hops * seam), BF)],
        (edge_count, ends, node_rows, edge_rows, edge_first),
        scalars=1,
        flops=7 * slots * unit,
        name="edge_local",
    )
    pre, hidden, normed, inv, agg, back0, back1 = call(
        edge_forward_kernel,
        [
            ((slots, features), F32),
            ((slots, features), BF),
            ((slots, features), F32),
            ((slots, 1), F32),
            ((verts, features), F32),
            seam32,
            seam32,
        ],
        (edge_count, ends, halo0, halo1, edge_rows, part, far, edge_first, edge_second),
        scalars=1,
        scratch=[(hops * seam, features)],
        flops=4 * slots * unit,
        name="edge_forward",
    )
    got0 = shift(back0, 1)
    got1 = shift(back1, 2)
    tall = (verts, features)
    new_nodes, agg16, node_hidden, d_out, d_pre, d_agg, out0, out1 = call(
        node_kernel,
        [(tall, BF)] * 6 + [seam16, seam16],
        (send_rows, node_rows, cot, agg, got0, got1, node_first, node_second),
        flops=8 * verts * unit,
        name="node",
    )
    d_halo0 = shift(out0, -1)
    d_halo1 = shift(out1, -2)
    node_grads, grad_part, up = call(
        fill_kernel,
        [((3 * features, features), BF), (tall, F32), ((slots, features), F32)],
        (node_rows, cot, agg16, node_hidden, d_out, d_pre, d_agg, node_first, pairs),
        flops=4 * slots * unit,
        name="fill",
    )
    grad_edges, pack, grad_part, back0, back1 = call(
        edge_backward_kernel,
        [
            ((slots, features), BF),
            ((2 * 7 * features, features // 2), BF),
            (tall, F32),
            seam32,
            seam32,
        ],
        (
            edge_count,
            ends,
            node_rows,
            halo0,
            halo1,
            edge_rows,
            up,
            far,
            d_halo0,
            d_halo1,
            pre,
            hidden,
            normed,
            inv,
            edge_first,
            edge_second,
            node_grads,
            grad_part,
        ),
        scalars=1,
        scratch=[tall, tall, (hops * seam, features), (features, features), (features, features)],
        flops=12 * slots * unit,
        name="edge_backward",
    )
    got0 = shift(back0, 1)
    got1 = shift(back1, 2)
    pack = sum_everywhere(pack)
    (grad_nodes,) = call(
        finish_kernel,
        [(tall, BF)],
        (send_rows, grad_part, got0, got1, edge_first),
        flops=verts * unit,
        name="finish",
    )
    grad_ef, grad_es, grad_nf, grad_ns = call(
        unpack_kernel,
        [
            ((3 * features, features), BF),
            ((features, features), BF),
            ((2 * features, features), BF),
            ((features, features), BF),
        ],
        (pack,),
        flops=1000,
        name="unpack",
    )
    return (
        new_nodes[None],
        grad_nodes[None],
        grad_edges[None],
        grad_ef,
        grad_es,
        grad_nf,
        grad_ns,
    )


def solution(mesh):
    fine = Mesh(mesh.devices.reshape(PATCH_SPLIT + (mesh.shape["rep"],)), PATCH + ("rep",))
    placed = (
        P("rep", PATCH, None),
        P("rep", PATCH, None),
        P(PATCH, None),
        P(PATCH),
        P(PATCH, None),
        P("rep", PATCH, None),
        P(),
        P(),
        P(),
        P(),
    )
    return jax.shard_map(
        local,
        mesh=fine,
        in_specs=placed,
        out_specs=(
            P("rep", PATCH, None),
            P("rep", PATCH, None),
            P("rep", PATCH, None),
            P(),
            P(),
            P(),
            P(),
        ),
        check_vma=False,
    )
```

```python
import jax
import jax.numpy as jnp
from jax import lax
from jax.experimental import pallas as pl
from jax.experimental.pallas import tpu as pltpu
from jax.sharding import Mesh, PartitionSpec as P

EPS = 1e-05
BF = jnp.bfloat16
F32 = jnp.float32
BLOCK = 512
PATCH_SPLIT = (4, 8, 2, 2)
PATCH = ("y", "zh", "zl", "c")
INNER = ("y", "zl", "c", "rep")
OUTER = ("zh",)


def dot(left, right):
    return jnp.dot(left, right, preferred_element_type=F32)


def dot_t(left, right):
    return lax.dot_general(left, right, (((1,), (1,)), ((), ())), preferred_element_type=F32)


def t_dot(left, right):
    return lax.dot_general(left, right, (((0,), (0,)), ((), ())), preferred_element_type=F32)


def split(values):
    high = values.astype(BF)
    return high, (values - high.astype(F32)).astype(BF)


def one_hot(index, shape, axis):
    return (index == lax.broadcasted_iota(jnp.int32, shape, axis)).astype(F32)


def normalize(values):
    centred = values - jnp.mean(values, axis=-1, keepdims=True)
    inv_scale = lax.rsqrt(jnp.mean(centred * centred, axis=-1, keepdims=True) + EPS)
    return centred * inv_scale, inv_scale


def norm_back(upstream, normed, inv_scale):
    return inv_scale * (
        upstream
        - jnp.mean(upstream, axis=-1, keepdims=True)
        - normed * jnp.mean(upstream * normed, axis=-1, keepdims=True)
    )


def sigmoid(pre):
    return 1.0 / (1.0 + jnp.exp(-pre))


def slope(pre):
    sigma = sigmoid(pre)
    return sigma * (1.0 + pre * (1.0 - sigma))


def live_row(ends_ref, row, start, count, offset=0):
    index = ends_ref[row : row + 1, pl.ds(start, BLOCK)]
    slot = start + lax.broadcasted_iota(jnp.int32, (1, BLOCK), 1)
    return jnp.where(slot < count, index - offset, -1)


def loop(total, body):
    def step(i, carry):
        body(pl.multiple_of(i * BLOCK, BLOCK))
        return carry

    lax.fori_loop(0, total // BLOCK, step, 0)


def seam_pick(send_ref, hop, table):
    verts = table.shape[0]
    slots = send_ref.shape[1]
    pick = one_hot(send_ref[hop : hop + 1, :], (verts, slots), 0).astype(BF)
    return t_dot(pick, table).astype(BF)


def seam_spread(send_ref, hop, verts, rows):
    slots = send_ref.shape[1]
    pick = one_hot(send_ref[hop : hop + 1, :], (verts, slots), 0)
    return jnp.dot(pick, rows, preferred_element_type=F32, precision=lax.Precision.HIGHEST)


def seam_kernel(send_ref, nodes_ref, out0_ref, out1_ref):
    table = nodes_ref[...]
    out0_ref[...] = seam_pick(send_ref, 0, table)
    out1_ref[...] = seam_pick(send_ref, 1, table)


def edge_local_kernel(
    count_ref, ends_ref, nodes_ref, edges_ref, ef_ref, pre_ref, pairs_ref, far_ref
):
    features = nodes_ref.shape[1]
    verts = nodes_ref.shape[0]
    seam = far_ref.shape[1]
    count = count_ref[0]

    def body(start):
        rows = pl.ds(start, BLOCK)
        first = live_row(ends_ref, 0, start, count)
        second = live_row(ends_ref, 1, start, count)
        both = jnp.concatenate([first, second, second, second, second, second, second, second], axis=0)
        cols = both.T
        first_col = cols[:, 0:1]
        second_col = cols[:, 1:2]
        pick_first = one_hot(first_col, (BLOCK, verts), 1)
        pick_second = one_hot(second_col, (BLOCK, verts), 1)
        far_ref[rows, :] = one_hot(second_col - verts, (BLOCK, seam), 1).astype(BF)
        pairs_ref[rows, :] = (pick_first + pick_second).astype(BF)
        table = nodes_ref[...]
        first_rows = dot(pick_first.astype(BF), table).astype(BF)
        second_rows = dot(pick_second.astype(BF), table).astype(BF)
        pre_ref[rows, :] = (
            dot(edges_ref[rows, :], ef_ref[:features, :])
            + dot(first_rows, ef_ref[features : 2 * features, :])
            + dot(second_rows, ef_ref[2 * features :, :])
        )

    loop(edges_ref.shape[0], body)


def edge_forward_kernel(
    count_ref,
    ends_ref,
    halo0_ref,
    halo1_ref,
    edges_ref,
    part_ref,
    far_ref,
    ef_ref,
    es_ref,
    pre_ref,
    hidden_ref,
    normed_ref,
    inv_ref,
    agg_ref,
    back0_ref,
    back1_ref,
    seam_ref,
):
    features = edges_ref.shape[1]
    verts = agg_ref.shape[0]
    slots = halo0_ref.shape[0]
    count = count_ref[0]
    halo = jnp.concatenate([halo0_ref[...], halo1_ref[...]], axis=0)
    agg_ref[...] = jnp.zeros_like(agg_ref)
    seam_ref[...] = jnp.zeros_like(seam_ref)

    def body(start):
        rows = pl.ds(start, BLOCK)
        far_rows = dot(far_ref[rows, :], halo).astype(BF)
        pre = part_ref[rows, :] + dot(far_rows, ef_ref[2 * features :, :])
        pre_ref[rows, :] = pre
        hidden = (pre * sigmoid(pre)).astype(BF)
        hidden_ref[rows, :] = hidden
        normed, inv = normalize(dot(hidden, es_ref[...]))
        normed_ref[rows, :] = normed
        inv_ref[rows, :] = inv
        new_edge = (edges_ref[rows, :].astype(F32) + normed).astype(BF)
        first = live_row(ends_ref, 0, start, count)
        second = live_row(ends_ref, 1, start, count)
        spread = one_hot(first, (verts, BLOCK), 0) + one_hot(second, (verts, BLOCK), 0)
        agg_ref[...] += dot(spread.astype(BF), new_edge)
        away = one_hot(second - verts, (2 * slots, BLOCK), 0).astype(BF)
        seam_ref[...] += dot(away, new_edge)

    loop(edges_ref.shape[0], body)
    back0_ref[...] = seam_ref[:slots, :]
    back1_ref[...] = seam_ref[slots:, :]


def node_kernel(
    send_ref,
    nodes_ref,
    cot_ref,
    agg_ref,
    got0_ref,
    got1_ref,
    nf_ref,
    ns_ref,
    new_ref,
    agg16_ref,
    hidden_ref,
    dout_ref,
    dpre_ref,
    dagg_ref,
    out0_ref,
    out1_ref,
):
    verts, features = nodes_ref.shape
    total = agg_ref[...] + seam_spread(send_ref, 0, verts, got0_ref[...])
    total = total + seam_spread(send_ref, 1, verts, got1_ref[...])
    aggregate = total.astype(BF)
    agg16_ref[...] = aggregate
    node_rows = nodes_ref[...]
    pre = dot(node_rows, nf_ref[:features, :]) + dot(aggregate, nf_ref[features:, :])
    sigma = sigmoid(pre)
    hidden = (pre * sigma).astype(BF)
    hidden_ref[...] = hidden
    normed, inv = normalize(dot(hidden, ns_ref[...]))
    new_ref[...] = (node_rows.astype(F32) + normed).astype(BF)
    d_out = norm_back(cot_ref[...].astype(F32), normed, inv).astype(BF)
    dout_ref[...] = d_out
    d_pre = (dot_t(d_out, ns_ref[...]) * (sigma * (1.0 + pre * (1.0 - sigma)))).astype(BF)
    dpre_ref[...] = d_pre
    d_agg = dot_t(d_pre, nf_ref[features:, :]).astype(BF)
    dagg_ref[...] = d_agg
    out0_ref[...] = seam_pick(send_ref, 0, d_agg)
    out1_ref[...] = seam_pick(send_ref, 1, d_agg)


def fill_kernel(
    nodes_ref,
    cot_ref,
    agg16_ref,
    hidden_ref,
    dout_ref,
    dpre_ref,
    dagg_ref,
    nf_ref,
    pairs_ref,
    grad_ref,
    part_ref,
    up_ref,
):
    features = nodes_ref.shape[1]
    d_pre = dpre_ref[...]

    def body(start):
        rows = pl.ds(start, BLOCK)
        up_ref[rows, :] = dot(pairs_ref[rows, :], dagg_ref[...])

    loop(pairs_ref.shape[0], body)
    grad_ref[:features, :] = t_dot(nodes_ref[...], d_pre).astype(BF)
    grad_ref[features : 2 * features, :] = t_dot(agg16_ref[...], d_pre).astype(BF)
    grad_ref[2 * features :, :] = t_dot(hidden_ref[...], dout_ref[...]).astype(BF)
    part_ref[...] = cot_ref[...].astype(F32) + dot_t(d_pre, nf_ref[:features, :])


def edge_backward_kernel(
    count_ref,
    ends_ref,
    nodes_ref,
    halo0_ref,
    halo1_ref,
    edges_ref,
    up_ref,
    far_ref,
    dhalo0_ref,
    dhalo1_ref,
    pre_ref,
    hidden_ref,
    normed_ref,
    inv_ref,
    ef_ref,
    es_ref,
    nodegrad_ref,
    part_ref,
    gedges_ref,
    pack_ref,
    partout_ref,
    back0_ref,
    back1_ref,
    first_ref,
    second_ref,
    seam_ref,
    ges_ref,
    ge1_ref,
):
    features = edges_ref.shape[1]
    half = features // 2
    verts = nodes_ref.shape[0]
    slots = halo0_ref.shape[0]
    count = count_ref[0]
    d_halo = jnp.concatenate([dhalo0_ref[...], dhalo1_ref[...]], axis=0)
    for ref in (first_ref, second_ref, seam_ref, ges_ref, ge1_ref):
        ref[...] = jnp.zeros_like(ref)

    def body(start):
        rows = pl.ds(start, BLOCK)
        up = up_ref[rows, :] + dot(far_ref[rows, :], d_halo)
        d_out = norm_back(up, normed_ref[rows, :], inv_ref[rows, :]).astype(BF)
        ges_ref[...] += t_dot(hidden_ref[rows, :], d_out)
        d_pre = (dot_t(d_out, es_ref[...]) * slope(pre_ref[rows, :])).astype(BF)
        first = live_row(ends_ref, 0, start, count)
        second = live_row(ends_ref, 1, start, count)
        seam_ref[...] += dot(one_hot(second - verts, (2 * slots, BLOCK), 0).astype(BF), d_pre)
        first_ref[...] += dot(one_hot(first, (verts, BLOCK), 0).astype(BF), d_pre)
        second_ref[...] += dot(one_hot(second, (verts, BLOCK), 0).astype(BF), d_pre)
        ge1_ref[...] += t_dot(edges_ref[rows, :], d_pre)
        gedges_ref[rows, :] = (up + dot_t(d_pre, ef_ref[:features, :])).astype(BF)

    loop(edges_ref.shape[0], body)
    back0_ref[...] = seam_ref[:slots, :]
    back1_ref[...] = seam_ref[slots:, :]
    total = pack_ref.shape[0] // 2

    def put(begin, grad):
        grad = grad.astype(BF)
        size = grad.shape[0]
        pack_ref[begin : begin + size, :] = grad[:, :half]
        pack_ref[total + begin : total + begin + size, :] = grad[:, half:]

    node_rows = nodes_ref[...]
    first_high, first_low = split(first_ref[...])
    second_high, second_low = split(second_ref[...])
    far_high, far_low = split(seam_ref[...])
    halo = jnp.concatenate([halo0_ref[...], halo1_ref[...]], axis=0)
    put(0, ge1_ref[...])
    put(features, t_dot(node_rows, first_high) + t_dot(node_rows, first_low))
    put(
        2 * features,
        t_dot(node_rows, second_high)
        + t_dot(node_rows, second_low)
        + t_dot(halo, far_high)
        + t_dot(halo, far_low),
    )
    put(3 * features, ges_ref[...])
    put(4 * features, nodegrad_ref[...])
    middle = ef_ref[features : 2 * features, :]
    last = ef_ref[2 * features :, :]
    partout_ref[...] = (
        part_ref[...]
        + (dot_t(first_high, middle) + dot_t(first_low, middle))
        + (dot_t(second_high, last) + dot_t(second_low, last))
    )


def finish_kernel(send_ref, part_ref, got0_ref, got1_ref, ef_ref, out_ref):
    verts, features = part_ref.shape
    last = ef_ref[2 * features :, :]
    total = part_ref[...]
    for hop, ref in enumerate((got0_ref, got1_ref)):
        high, low = split(ref[...])
        total = total + seam_spread(send_ref, hop, verts, dot_t(high, last) + dot_t(low, last))
    out_ref[...] = total.astype(BF)


def unpack_kernel(pack_ref, gef_ref, ges_ref, gnf_ref, gns_ref):
    total = pack_ref.shape[0] // 2
    half = pack_ref.shape[1]
    begin = 0
    for ref in (gef_ref, ges_ref, gnf_ref, gns_ref):
        size = ref.shape[0]
        ref[:, :half] = pack_ref[begin : begin + size, :]
        ref[:, half:] = pack_ref[total + begin : total + begin + size, :]
        begin += size


def call(kernel, outs, args, scalars=0, scratch=(), flops=0, name=None):
    return pl.pallas_call(
        kernel,
        out_shape=[jax.ShapeDtypeStruct(shape, kind) for shape, kind in outs],
        in_specs=[
            pl.BlockSpec(memory_space=pltpu.SMEM if i < scalars else pltpu.VMEM)
            for i in range(len(args))
        ],
        out_specs=[pl.BlockSpec(memory_space=pltpu.VMEM) for _ in outs],
        scratch_shapes=[pltpu.VMEM(shape, F32) for shape in scratch],
        compiler_params=pltpu.CompilerParams(vmem_limit_bytes=24 * 2**20),
        cost_estimate=pl.CostEstimate(flops=flops, transcendentals=0, bytes_accessed=flops // 1000),
        name=name,
    )(*args)


def shift(block, distance):
    count = lax.axis_size(PATCH)
    return lax.ppermute(block, PATCH, [((i - distance) % count, i) for i in range(count)])


def group_size(axes):
    return lax.axis_size(axes)


def sum_everywhere(pack):
    inner = group_size(INNER)
    outer = group_size(OUTER)
    rows, lanes = pack.shape
    pieces = lax.all_to_all(pack.reshape(inner, rows // inner, lanes), INNER, 0, 0)
    mine = jnp.sum(pieces.astype(F32), axis=0).astype(BF)
    spread = jnp.broadcast_to(mine[None], (outer,) + mine.shape)
    pieces = lax.all_to_all(spread, OUTER, 0, 0)
    mine = jnp.sum(pieces.astype(F32), axis=0).astype(BF)
    spread = jnp.broadcast_to(mine[None], (inner,) + mine.shape)
    return lax.all_to_all(spread, INNER, 0, 0).reshape(rows, lanes)


def local(
    nodes,
    edges,
    edge_ends,
    edge_count,
    send_rows,
    cotangent,
    edge_first,
    edge_second,
    node_first,
    node_second,
):
    node_rows = nodes[0]
    edge_rows = edges[0]
    cot = cotangent[0]
    verts, features = node_rows.shape
    slots = edge_rows.shape[0]
    hops, seam = send_rows.shape
    assert hops == 2
    ends = edge_ends.T
    seam16 = ((seam, features), BF)
    seam32 = ((seam, features), F32)
    unit = 2 * features * features

    out0, out1 = call(seam_kernel, [seam16, seam16], (send_rows, node_rows), flops=10**8, name="seam")
    halo0 = shift(out0, -1)
    halo1 = shift(out1, -2)
    part, pairs, far = call(
        edge_local_kernel,
        [((slots, features), F32), ((slots, verts), BF), ((slots, hops * seam), BF)],
        (edge_count, ends, node_rows, edge_rows, edge_first),
        scalars=1,
        flops=7 * slots * unit,
        name="edge_local",
    )
    pre, hidden, normed, inv, agg, back0, back1 = call(
        edge_forward_kernel,
        [
            ((slots, features), F32),
            ((slots, features), BF),
            ((slots, features), F32),
            ((slots, 1), F32),
            ((verts, features), F32),
            seam32,
            seam32,
        ],
        (edge_count, ends, halo0, halo1, edge_rows, part, far, edge_first, edge_second),
        scalars=1,
        scratch=[(hops * seam, features)],
        flops=4 * slots * unit,
        name="edge_forward",
    )
    got0 = shift(back0, 1)
    got1 = shift(back1, 2)
    tall = (verts, features)
    new_nodes, agg16, node_hidden, d_out, d_pre, d_agg, out0, out1 = call(
        node_kernel,
        [(tall, BF)] * 6 + [seam16, seam16],
        (send_rows, node_rows, cot, agg, got0, got1, node_first, node_second),
        flops=8 * verts * unit,
        name="node",
    )
    d_halo0 = shift(out0, -1)
    d_halo1 = shift(out1, -2)
    node_grads, grad_part, up = call(
        fill_kernel,
        [((3 * features, features), BF), (tall, F32), ((slots, features), F32)],
        (node_rows, cot, agg16, node_hidden, d_out, d_pre, d_agg, node_first, pairs),
        flops=4 * slots * unit,
        name="fill",
    )
    grad_edges, pack, grad_part, back0, back1 = call(
        edge_backward_kernel,
        [
            ((slots, features), BF),
            ((2 * 7 * features, features // 2), BF),
            (tall, F32),
            seam32,
            seam32,
        ],
        (
            edge_count,
            ends,
            node_rows,
            halo0,
            halo1,
            edge_rows,
            up,
            far,
            d_halo0,
            d_halo1,
            pre,
            hidden,
            normed,
            inv,
            edge_first,
            edge_second,
            node_grads,
            grad_part,
        ),
        scalars=1,
        scratch=[tall, tall, (hops * seam, features), (features, features), (features, features)],
        flops=12 * slots * unit,
        name="edge_backward",
    )
    got0 = shift(back0, 1)
    got1 = shift(back1, 2)
    pack = sum_everywhere(pack)
    (grad_nodes,) = call(
        finish_kernel,
        [(tall, BF)],
        (send_rows, grad_part, got0, got1, edge_first),
        flops=verts * unit,
        name="finish",
    )
    grad_ef, grad_es, grad_nf, grad_ns = call(
        unpack_kernel,
        [
            ((3 * features, features), BF),
            ((features, features), BF),
            ((2 * features, features), BF),
            ((features, features), BF),
        ],
        (pack,),
        flops=1000,
        name="unpack",
    )
    return (
        new_nodes[None],
        grad_nodes[None],
        grad_edges[None],
        grad_ef,
        grad_es,
        grad_nf,
        grad_ns,
    )


def solution(mesh):
    fine = Mesh(mesh.devices.reshape(PATCH_SPLIT + (mesh.shape["rep"],)), PATCH + ("rep",))
    placed = (
        P("rep", PATCH, None),
        P("rep", PATCH, None),
        P(PATCH, None),
        P(PATCH),
        P(PATCH, None),
        P("rep", PATCH, None),
        P(),
        P(),
        P(),
        P(),
    )
    return jax.shard_map(
        local,
        mesh=fine,
        in_specs=placed,
        out_specs=(
            P("rep", PATCH, None),
            P("rep", PATCH, None),
            P("rep", PATCH, None),
            P(),
            P(),
            P(),
            P(),
        ),
        check_vma=False,
    )
```

```python
import jax
import jax.numpy as jnp
from jax import lax
from jax.experimental import pallas as pl
from jax.experimental.pallas import tpu as pltpu
from jax.sharding import Mesh, PartitionSpec as P

EPS = 1e-05
BF = jnp.bfloat16
F32 = jnp.float32
BLOCK = 512
PATCH_SPLIT = (4, 8, 2, 2)
PATCH = ("y", "zh", "zl", "c")
INNER = ("y", "zl", "c", "rep")
OUTER = ("zh",)


def dot(left, right):
    return jnp.dot(left, right, preferred_element_type=F32)


def dot_t(left, right):
    return lax.dot_general(left, right, (((1,), (1,)), ((), ())), preferred_element_type=F32)


def t_dot(left, right):
    return lax.dot_general(left, right, (((0,), (0,)), ((), ())), preferred_element_type=F32)


def split(values):
    high = values.astype(BF)
    return high, (values - high.astype(F32)).astype(BF)


def one_hot(index, shape, axis):
    return (index == lax.broadcasted_iota(jnp.int32, shape, axis)).astype(F32)


def normalize(values):
    centred = values - jnp.mean(values, axis=-1, keepdims=True)
    inv_scale = lax.rsqrt(jnp.mean(centred * centred, axis=-1, keepdims=True) + EPS)
    return centred * inv_scale, inv_scale


def norm_back(upstream, normed, inv_scale):
    return inv_scale * (
        upstream
        - jnp.mean(upstream, axis=-1, keepdims=True)
        - normed * jnp.mean(upstream * normed, axis=-1, keepdims=True)
    )


def sigmoid(pre):
    return 1.0 / (1.0 + jnp.exp(-pre))


def slope(pre):
    sigma = sigmoid(pre)
    return sigma * (1.0 + pre * (1.0 - sigma))


def live_row(ends_ref, row, start, count, offset=0):
    index = ends_ref[row : row + 1, pl.ds(start, BLOCK)]
    slot = start + lax.broadcasted_iota(jnp.int32, (1, BLOCK), 1)
    return jnp.where(slot < count, index - offset, -1)


def loop(total, body):
    def step(i, carry):
        body(pl.multiple_of(i * BLOCK, BLOCK))
        return carry

    lax.fori_loop(0, total // BLOCK, step, 0)


def seam_pick(send_ref, hop, table):
    verts = table.shape[0]
    slots = send_ref.shape[1]
    pick = one_hot(send_ref[hop : hop + 1, :], (verts, slots), 0).astype(BF)
    return t_dot(pick, table).astype(BF)


def seam_spread(send_ref, hop, verts, rows):
    slots = send_ref.shape[1]
    pick = one_hot(send_ref[hop : hop + 1, :], (verts, slots), 0)
    return jnp.dot(pick, rows, preferred_element_type=F32, precision=lax.Precision.HIGHEST)


def load_kernel(
    send_hbm,
    nodes_hbm,
    ends_hbm,
    ef_hbm,
    edges_hbm,
    out0_ref,
    out1_ref,
    send_ref,
    nodes_ref,
    ends_ref,
    ef_ref,
    edges_ref,
    sems,
):
    sources = (send_hbm, nodes_hbm, ends_hbm, ef_hbm, edges_hbm)
    targets = (send_ref, nodes_ref, ends_ref, ef_ref, edges_ref)
    copies = [
        pltpu.make_async_copy(source, target, sems.at[i])
        for i, (source, target) in enumerate(zip(sources, targets))
    ]
    for copy in copies:
        copy.start()
    copies[0].wait()
    copies[1].wait()
    table = nodes_ref[...]
    out0_ref[...] = seam_pick(send_ref, 0, table)
    out1_ref[...] = seam_pick(send_ref, 1, table)
    for copy in copies[2:]:
        copy.wait()


def load(sources):
    send, nodes = sources[:2]
    seam = jax.ShapeDtypeStruct((send.shape[1], nodes.shape[1]), BF)
    return pl.pallas_call(
        load_kernel,
        out_shape=[seam, seam] + [jax.ShapeDtypeStruct(x.shape, x.dtype) for x in sources],
        in_specs=[pl.BlockSpec(memory_space=pltpu.HBM) for _ in sources],
        out_specs=[pl.BlockSpec(memory_space=pltpu.VMEM) for _ in range(2 + len(sources))],
        scratch_shapes=[pltpu.SemaphoreType.DMA((len(sources),))],
        compiler_params=pltpu.CompilerParams(vmem_limit_bytes=24 * 2**20),
        cost_estimate=pl.CostEstimate(flops=10**8, transcendentals=0, bytes_accessed=10**6),
        name="load",
    )(*[pltpu.with_memory_space_constraint(x, pltpu.HBM) for x in sources])


def edge_local_kernel(
    count_ref, ends_ref, nodes_ref, edges_ref, ef_ref, pre_ref, pairs_ref, far_ref
):
    features = nodes_ref.shape[1]
    verts = nodes_ref.shape[0]
    seam = far_ref.shape[1]
    count = count_ref[0]

    def body(start):
        rows = pl.ds(start, BLOCK)
        first = live_row(ends_ref, 0, start, count)
        second = live_row(ends_ref, 1, start, count)
        both = jnp.concatenate([first, second, second, second, second, second, second, second], axis=0)
        cols = both.T
        first_col = cols[:, 0:1]
        second_col = cols[:, 1:2]
        pick_first = one_hot(first_col, (BLOCK, verts), 1)
        pick_second = one_hot(second_col, (BLOCK, verts), 1)
        far_ref[rows, :] = one_hot(second_col - verts, (BLOCK, seam), 1).astype(BF)
        pairs_ref[rows, :] = (pick_first + pick_second).astype(BF)
        table = nodes_ref[...]
        first_rows = dot(pick_first.astype(BF), table).astype(BF)
        second_rows = dot(pick_second.astype(BF), table).astype(BF)
        pre_ref[rows, :] = (
            dot(edges_ref[rows, :], ef_ref[:features, :])
            + dot(first_rows, ef_ref[features : 2 * features, :])
            + dot(second_rows, ef_ref[2 * features :, :])
        )

    loop(edges_ref.shape[0], body)


def edge_forward_kernel(
    count_ref,
    ends_ref,
    halo0_ref,
    halo1_ref,
    edges_ref,
    part_ref,
    far_ref,
    ef_ref,
    es_ref,
    pre_ref,
    hidden_ref,
    normed_ref,
    inv_ref,
    agg_ref,
    back0_ref,
    back1_ref,
    seam_ref,
):
    features = edges_ref.shape[1]
    verts = agg_ref.shape[0]
    slots = halo0_ref.shape[0]
    count = count_ref[0]
    halo = jnp.concatenate([halo0_ref[...], halo1_ref[...]], axis=0)
    agg_ref[...] = jnp.zeros_like(agg_ref)
    seam_ref[...] = jnp.zeros_like(seam_ref)

    def body(start):
        rows = pl.ds(start, BLOCK)
        far_rows = dot(far_ref[rows, :], halo).astype(BF)
        pre = part_ref[rows, :] + dot(far_rows, ef_ref[2 * features :, :])
        pre_ref[rows, :] = pre
        hidden = (pre * sigmoid(pre)).astype(BF)
        hidden_ref[rows, :] = hidden
        normed, inv = normalize(dot(hidden, es_ref[...]))
        normed_ref[rows, :] = normed
        inv_ref[rows, :] = inv
        new_edge = (edges_ref[rows, :].astype(F32) + normed).astype(BF)
        first = live_row(ends_ref, 0, start, count)
        second = live_row(ends_ref, 1, start, count)
        spread = one_hot(first, (verts, BLOCK), 0) + one_hot(second, (verts, BLOCK), 0)
        agg_ref[...] += dot(spread.astype(BF), new_edge)
        away = one_hot(second - verts, (2 * slots, BLOCK), 0).astype(BF)
        seam_ref[...] += dot(away, new_edge)

    loop(edges_ref.shape[0], body)
    back0_ref[...] = seam_ref[:slots, :]
    back1_ref[...] = seam_ref[slots:, :]


def node_kernel(
    send_ref,
    nodes_ref,
    cot_ref,
    agg_ref,
    got0_ref,
    got1_ref,
    nf_ref,
    ns_ref,
    new_ref,
    agg16_ref,
    hidden_ref,
    dout_ref,
    dpre_ref,
    dagg_ref,
    out0_ref,
    out1_ref,
):
    verts, features = nodes_ref.shape
    total = agg_ref[...] + seam_spread(send_ref, 0, verts, got0_ref[...])
    total = total + seam_spread(send_ref, 1, verts, got1_ref[...])
    aggregate = total.astype(BF)
    agg16_ref[...] = aggregate
    node_rows = nodes_ref[...]
    pre = dot(node_rows, nf_ref[:features, :]) + dot(aggregate, nf_ref[features:, :])
    sigma = sigmoid(pre)
    hidden = (pre * sigma).astype(BF)
    hidden_ref[...] = hidden
    normed, inv = normalize(dot(hidden, ns_ref[...]))
    new_ref[...] = (node_rows.astype(F32) + normed).astype(BF)
    d_out = norm_back(cot_ref[...].astype(F32), normed, inv).astype(BF)
    dout_ref[...] = d_out
    d_pre = (dot_t(d_out, ns_ref[...]) * (sigma * (1.0 + pre * (1.0 - sigma)))).astype(BF)
    dpre_ref[...] = d_pre
    d_agg = dot_t(d_pre, nf_ref[features:, :]).astype(BF)
    dagg_ref[...] = d_agg
    out0_ref[...] = seam_pick(send_ref, 0, d_agg)
    out1_ref[...] = seam_pick(send_ref, 1, d_agg)


def fill_kernel(
    nodes_ref,
    cot_ref,
    agg16_ref,
    hidden_ref,
    dout_ref,
    dpre_ref,
    dagg_ref,
    nf_ref,
    pairs_ref,
    grad_ref,
    part_ref,
    up_ref,
):
    features = nodes_ref.shape[1]
    d_pre = dpre_ref[...]

    def body(start):
        rows = pl.ds(start, BLOCK)
        up_ref[rows, :] = dot(pairs_ref[rows, :], dagg_ref[...])

    loop(pairs_ref.shape[0], body)
    grad_ref[:features, :] = t_dot(nodes_ref[...], d_pre).astype(BF)
    grad_ref[features : 2 * features, :] = t_dot(agg16_ref[...], d_pre).astype(BF)
    grad_ref[2 * features :, :] = t_dot(hidden_ref[...], dout_ref[...]).astype(BF)
    part_ref[...] = cot_ref[...].astype(F32) + dot_t(d_pre, nf_ref[:features, :])


def edge_backward_kernel(
    count_ref,
    ends_ref,
    nodes_ref,
    halo0_ref,
    halo1_ref,
    edges_ref,
    up_ref,
    far_ref,
    dhalo0_ref,
    dhalo1_ref,
    pre_ref,
    hidden_ref,
    normed_ref,
    inv_ref,
    ef_ref,
    es_ref,
    nodegrad_ref,
    part_ref,
    gedges_ref,
    pack_ref,
    partout_ref,
    back0_ref,
    back1_ref,
    first_ref,
    second_ref,
    seam_ref,
    ges_ref,
    ge1_ref,
):
    features = edges_ref.shape[1]
    half = features // 2
    verts = nodes_ref.shape[0]
    slots = halo0_ref.shape[0]
    count = count_ref[0]
    d_halo = jnp.concatenate([dhalo0_ref[...], dhalo1_ref[...]], axis=0)
    for ref in (first_ref, second_ref, seam_ref, ges_ref, ge1_ref):
        ref[...] = jnp.zeros_like(ref)

    def body(start):
        rows = pl.ds(start, BLOCK)
        up = up_ref[rows, :] + dot(far_ref[rows, :], d_halo)
        d_out = norm_back(up, normed_ref[rows, :], inv_ref[rows, :]).astype(BF)
        ges_ref[...] += t_dot(hidden_ref[rows, :], d_out)
        d_pre = (dot_t(d_out, es_ref[...]) * slope(pre_ref[rows, :])).astype(BF)
        first = live_row(ends_ref, 0, start, count)
        second = live_row(ends_ref, 1, start, count)
        seam_ref[...] += dot(one_hot(second - verts, (2 * slots, BLOCK), 0).astype(BF), d_pre)
        first_ref[...] += dot(one_hot(first, (verts, BLOCK), 0).astype(BF), d_pre)
        second_ref[...] += dot(one_hot(second, (verts, BLOCK), 0).astype(BF), d_pre)
        ge1_ref[...] += t_dot(edges_ref[rows, :], d_pre)
        gedges_ref[rows, :] = (up + dot_t(d_pre, ef_ref[:features, :])).astype(BF)

    loop(edges_ref.shape[0], body)
    back0_ref[...] = seam_ref[:slots, :]
    back1_ref[...] = seam_ref[slots:, :]
    total = pack_ref.shape[0] // 2

    def put(begin, grad):
        grad = grad.astype(BF)
        size = grad.shape[0]
        pack_ref[begin : begin + size, :] = grad[:, :half]
        pack_ref[total + begin : total + begin + size, :] = grad[:, half:]

    node_rows = nodes_ref[...]
    first_high, first_low = split(first_ref[...])
    second_high, second_low = split(second_ref[...])
    far_high, far_low = split(seam_ref[...])
    halo = jnp.concatenate([halo0_ref[...], halo1_ref[...]], axis=0)
    put(0, ge1_ref[...])
    put(features, t_dot(node_rows, first_high) + t_dot(node_rows, first_low))
    put(
        2 * features,
        t_dot(node_rows, second_high)
        + t_dot(node_rows, second_low)
        + t_dot(halo, far_high)
        + t_dot(halo, far_low),
    )
    put(3 * features, ges_ref[...])
    put(4 * features, nodegrad_ref[...])
    middle = ef_ref[features : 2 * features, :]
    last = ef_ref[2 * features :, :]
    partout_ref[...] = (
        part_ref[...]
        + (dot_t(first_high, middle) + dot_t(first_low, middle))
        + (dot_t(second_high, last) + dot_t(second_low, last))
    )


def finish_kernel(send_ref, part_ref, got0_ref, got1_ref, ef_ref, out_ref):
    verts, features = part_ref.shape
    last = ef_ref[2 * features :, :]
    total = part_ref[...]
    for hop, ref in enumerate((got0_ref, got1_ref)):
        high, low = split(ref[...])
        total = total + seam_spread(send_ref, hop, verts, dot_t(high, last) + dot_t(low, last))
    out_ref[...] = total.astype(BF)


def unpack_kernel(pack_ref, gef_ref, ges_ref, gnf_ref, gns_ref):
    total = pack_ref.shape[0] // 2
    half = pack_ref.shape[1]
    begin = 0
    for ref in (gef_ref, ges_ref, gnf_ref, gns_ref):
        size = ref.shape[0]
        ref[:, :half] = pack_ref[begin : begin + size, :]
        ref[:, half:] = pack_ref[total + begin : total + begin + size, :]
        begin += size


def call(kernel, outs, args, scalars=0, scratch=(), flops=0, name=None):
    return pl.pallas_call(
        kernel,
        out_shape=[jax.ShapeDtypeStruct(shape, kind) for shape, kind in outs],
        in_specs=[
            pl.BlockSpec(memory_space=pltpu.SMEM if i < scalars else pltpu.VMEM)
            for i in range(len(args))
        ],
        out_specs=[pl.BlockSpec(memory_space=pltpu.VMEM) for _ in outs],
        scratch_shapes=[pltpu.VMEM(shape, F32) for shape in scratch],
        compiler_params=pltpu.CompilerParams(vmem_limit_bytes=24 * 2**20),
        cost_estimate=pl.CostEstimate(flops=flops, transcendentals=0, bytes_accessed=flops // 1000),
        name=name,
    )(*args)


def shift(block, distance):
    count = lax.axis_size(PATCH)
    return lax.ppermute(block, PATCH, [((i - distance) % count, i) for i in range(count)])


def group_size(axes):
    return lax.axis_size(axes)


def sum_kernel(pieces_ref, out_ref):
    count = pieces_ref.shape[0]
    copies = out_ref.shape[0]
    total = lax.fori_loop(
        1,
        count,
        lambda i, acc: acc + pieces_ref[i].astype(F32),
        pieces_ref[0].astype(F32),
        unroll=7,
    ).astype(BF)

    def store(i, carry):
        out_ref[i] = total
        return carry

    lax.fori_loop(0, copies, store, 0, unroll=8)


def sum_and_copy(pieces, copies, name):
    (out,) = call(
        sum_kernel, [((copies,) + pieces.shape[1:], BF)], (pieces,), flops=pieces.size, name=name
    )
    return out


def sum_everywhere(pack):
    inner = group_size(INNER)
    outer = group_size(OUTER)
    rows, lanes = pack.shape
    pieces = lax.all_to_all(pack.reshape(inner, rows // inner, lanes), INNER, 0, 0)
    pieces = lax.all_to_all(sum_and_copy(pieces, outer, "inner_sum"), OUTER, 0, 0)
    pieces = lax.all_to_all(sum_and_copy(pieces, inner, "outer_sum"), INNER, 0, 0)
    return pieces.reshape(rows, lanes)


def local(
    nodes,
    edges,
    edge_ends,
    edge_count,
    send_rows,
    cotangent,
    edge_first,
    edge_second,
    node_first,
    node_second,
):
    node_rows = nodes[0]
    edge_rows = edges[0]
    cot = cotangent[0]
    verts, features = node_rows.shape
    slots = edge_rows.shape[0]
    hops, seam = send_rows.shape
    assert hops == 2
    ends = edge_ends.T
    seam16 = ((seam, features), BF)
    seam32 = ((seam, features), F32)
    unit = 2 * features * features

    out0, out1, send_rows, node_rows, ends, edge_first, edge_rows = load(
        (send_rows, node_rows, ends, edge_first, edge_rows)
    )
    halo0 = shift(out0, -1)
    halo1 = shift(out1, -2)
    part, pairs, far = call(
        edge_local_kernel,
        [((slots, features), F32), ((slots, verts), BF), ((slots, hops * seam), BF)],
        (edge_count, ends, node_rows, edge_rows, edge_first),
        scalars=1,
        flops=7 * slots * unit,
        name="edge_local",
    )
    pre, hidden, normed, inv, agg, back0, back1 = call(
        edge_forward_kernel,
        [
            ((slots, features), F32),
            ((slots, features), BF),
            ((slots, features), F32),
            ((slots, 1), F32),
            ((verts, features), F32),
            seam32,
            seam32,
        ],
        (edge_count, ends, halo0, halo1, edge_rows, part, far, edge_first, edge_second),
        scalars=1,
        scratch=[(hops * seam, features)],
        flops=4 * slots * unit,
        name="edge_forward",
    )
    got0 = shift(back0, 1)
    got1 = shift(back1, 2)
    tall = (verts, features)
    new_nodes, agg16, node_hidden, d_out, d_pre, d_agg, out0, out1 = call(
        node_kernel,
        [(tall, BF)] * 6 + [seam16, seam16],
        (send_rows, node_rows, cot, agg, got0, got1, node_first, node_second),
        flops=8 * verts * unit,
        name="node",
    )
    d_halo0 = shift(out0, -1)
    d_halo1 = shift(out1, -2)
    node_grads, grad_part, up = call(
        fill_kernel,
        [((3 * features, features), BF), (tall, F32), ((slots, features), F32)],
        (node_rows, cot, agg16, node_hidden, d_out, d_pre, d_agg, node_first, pairs),
        flops=4 * slots * unit,
        name="fill",
    )
    grad_edges, pack, grad_part, back0, back1 = call(
        edge_backward_kernel,
        [
            ((slots, features), BF),
            ((2 * 7 * features, features // 2), BF),
            (tall, F32),
            seam32,
            seam32,
        ],
        (
            edge_count,
            ends,
            node_rows,
            halo0,
            halo1,
            edge_rows,
            up,
            far,
            d_halo0,
            d_halo1,
            pre,
            hidden,
            normed,
            inv,
            edge_first,
            edge_second,
            node_grads,
            grad_part,
        ),
        scalars=1,
        scratch=[tall, tall, (hops * seam, features), (features, features), (features, features)],
        flops=12 * slots * unit,
        name="edge_backward",
    )
    got0 = shift(back0, 1)
    got1 = shift(back1, 2)
    pack = sum_everywhere(pack)
    (grad_nodes,) = call(
        finish_kernel,
        [(tall, BF)],
        (send_rows, grad_part, got0, got1, edge_first),
        flops=verts * unit,
        name="finish",
    )
    grad_ef, grad_es, grad_nf, grad_ns = call(
        unpack_kernel,
        [
            ((3 * features, features), BF),
            ((features, features), BF),
            ((2 * features, features), BF),
            ((features, features), BF),
        ],
        (pack,),
        flops=1000,
        name="unpack",
    )
    return (
        new_nodes[None],
        grad_nodes[None],
        grad_edges[None],
        grad_ef,
        grad_es,
        grad_nf,
        grad_ns,
    )


def solution(mesh):
    fine = Mesh(mesh.devices.reshape(PATCH_SPLIT + (mesh.shape["rep"],)), PATCH + ("rep",))
    placed = (
        P("rep", PATCH, None),
        P("rep", PATCH, None),
        P(PATCH, None),
        P(PATCH),
        P(PATCH, None),
        P("rep", PATCH, None),
        P(),
        P(),
        P(),
        P(),
    )
    return jax.shard_map(
        local,
        mesh=fine,
        in_specs=placed,
        out_specs=(
            P("rep", PATCH, None),
            P("rep", PATCH, None),
            P("rep", PATCH, None),
            P(),
            P(),
            P(),
            P(),
        ),
        check_vma=False,
    )
```

```python
import functools

import jax
import jax.numpy as jnp
from jax import lax
from jax.experimental import pallas as pl
from jax.experimental.pallas import tpu as pltpu
from jax.sharding import Mesh, PartitionSpec as P

EPS = 1e-05
BF = jnp.bfloat16
F32 = jnp.float32
BLOCK = 1536
PATCH_SPLIT = (4, 8, 2, 2)
PATCH = ("y", "zh", "zl", "c")
INNER = ("y", "zl", "c", "rep")
OUTER = ("zh",)


def dot(left, right):
    return jnp.dot(left, right, preferred_element_type=F32)


def dot_t(left, right):
    return lax.dot_general(left, right, (((1,), (1,)), ((), ())), preferred_element_type=F32)


def t_dot(left, right):
    return lax.dot_general(left, right, (((0,), (0,)), ((), ())), preferred_element_type=F32)


def split(values):
    high = values.astype(BF)
    return high, (values - high.astype(F32)).astype(BF)


def one_hot(index, shape, axis):
    return (index == lax.broadcasted_iota(jnp.int32, shape, axis)).astype(F32)


def normalize(values):
    centred = values - jnp.mean(values, axis=-1, keepdims=True)
    inv_scale = lax.rsqrt(jnp.mean(centred * centred, axis=-1, keepdims=True) + EPS)
    return centred * inv_scale, inv_scale


def norm_back(upstream, normed, inv_scale):
    return inv_scale * (
        upstream
        - jnp.mean(upstream, axis=-1, keepdims=True)
        - normed * jnp.mean(upstream * normed, axis=-1, keepdims=True)
    )


def sigmoid(pre):
    return 1.0 / (1.0 + jnp.exp(-pre))


def slope(pre):
    sigma = sigmoid(pre)
    return sigma * (1.0 + pre * (1.0 - sigma))


def live_row(ends_ref, row, start, count, offset=0):
    index = ends_ref[row : row + 1, pl.ds(start, BLOCK)]
    slot = start + lax.broadcasted_iota(jnp.int32, (1, BLOCK), 1)
    return jnp.where(slot < count, index - offset, -1)


def loop(total, body):
    def step(i, carry):
        body(pl.multiple_of(i * BLOCK, BLOCK))
        return carry

    lax.fori_loop(0, total // BLOCK, step, 0)


def seam_tables(send_ref, pick_ref, spread_ref):
    hops, slots = send_ref.shape
    wide, verts = pick_ref.shape
    flat = jnp.concatenate([send_ref[hop : hop + 1, :] for hop in range(hops)], axis=1)
    spread = one_hot(flat, (verts, wide), 0)
    spread_ref[...] = jnp.concatenate([spread, spread], axis=1).astype(BF)
    column = jnp.broadcast_to(flat, (8, wide)).T[:, 0:1]
    pick_ref[...] = one_hot(column, (wide, verts), 1).astype(BF)


def seam_spread(spread_ref, rows):
    high, low = split(rows)
    return dot(spread_ref[...], jnp.concatenate([high, low], axis=0))


def load_kernel(
    send_hbm,
    nodes_hbm,
    ends_hbm,
    ef_hbm,
    edges_hbm,
    out0_ref,
    out1_ref,
    nodes_ref,
    ends_ref,
    ef_ref,
    edges_ref,
    pick_ref,
    spread_ref,
    send_ref,
    sems,
):
    sources = (send_hbm, nodes_hbm, ends_hbm, ef_hbm, edges_hbm)
    targets = (send_ref, nodes_ref, ends_ref, ef_ref, edges_ref)
    copies = [
        pltpu.make_async_copy(source, target, sems.at[i])
        for i, (source, target) in enumerate(zip(sources, targets))
    ]
    for copy in copies:
        copy.start()
    copies[0].wait()
    seam_tables(send_ref, pick_ref, spread_ref)
    copies[1].wait()
    picked = dot(pick_ref[...], nodes_ref[...]).astype(BF)
    slots = out0_ref.shape[0]
    out0_ref[...] = picked[:slots]
    out1_ref[...] = picked[slots:]
    for copy in copies[2:]:
        copy.wait()


def load(sources):
    send, nodes = sources[:2]
    wide = send.shape[0] * send.shape[1]
    outs = [jax.ShapeDtypeStruct(x.shape, x.dtype) for x in sources[1:]]
    outs.append(jax.ShapeDtypeStruct((wide, nodes.shape[0]), BF))
    outs.append(jax.ShapeDtypeStruct((nodes.shape[0], 2 * wide), BF))
    seam = jax.ShapeDtypeStruct((send.shape[1], nodes.shape[1]), BF)
    return pl.pallas_call(
        load_kernel,
        out_shape=[seam, seam] + outs,
        in_specs=[pl.BlockSpec(memory_space=pltpu.HBM) for _ in sources],
        out_specs=[pl.BlockSpec(memory_space=pltpu.VMEM) for _ in range(2 + len(outs))],
        scratch_shapes=[
            pltpu.VMEM(send.shape, send.dtype),
            pltpu.SemaphoreType.DMA((len(sources),)),
        ],
        compiler_params=pltpu.CompilerParams(vmem_limit_bytes=24 * 2**20),
        cost_estimate=pl.CostEstimate(flops=10**8, transcendentals=0, bytes_accessed=10**6),
        name="load",
    )(*[pltpu.with_memory_space_constraint(x, pltpu.HBM) for x in sources])


def edge_local_kernel(
    count_ref, ends_ref, nodes_ref, edges_ref, ef_ref, pre_ref, pairs_ref, far_ref
):
    features = nodes_ref.shape[1]
    verts = nodes_ref.shape[0]
    seam = far_ref.shape[1]
    count = count_ref[0]

    def body(start):
        rows = pl.ds(start, BLOCK)
        first = live_row(ends_ref, 0, start, count)
        second = live_row(ends_ref, 1, start, count)
        both = jnp.concatenate([first, second, second, second, second, second, second, second], axis=0)
        cols = both.T
        first_col = cols[:, 0:1]
        second_col = cols[:, 1:2]
        pick_first = one_hot(first_col, (BLOCK, verts), 1)
        pick_second = one_hot(second_col, (BLOCK, verts), 1)
        far_ref[rows, :] = one_hot(second_col - verts, (BLOCK, seam), 1).astype(BF)
        pairs_ref[rows, :] = (pick_first + pick_second).astype(BF)
        table = nodes_ref[...]
        first_rows = dot(pick_first.astype(BF), table).astype(BF)
        second_rows = dot(pick_second.astype(BF), table).astype(BF)
        pre_ref[rows, :] = (
            dot(edges_ref[rows, :], ef_ref[:features, :])
            + dot(first_rows, ef_ref[features : 2 * features, :])
            + dot(second_rows, ef_ref[2 * features :, :])
        )

    loop(edges_ref.shape[0], body)


def aggregate_kernel(count_ref, ends_ref, new_ref, agg_ref):
    verts = agg_ref.shape[0]
    count = count_ref[0]
    agg_ref[...] = jnp.zeros_like(agg_ref)

    def body(start):
        first = live_row(ends_ref, 0, start, count)
        second = live_row(ends_ref, 1, start, count)
        spread = one_hot(first, (verts, BLOCK), 0) + one_hot(second, (verts, BLOCK), 0)
        agg_ref[...] += dot(spread.astype(BF), new_ref[pl.ds(start, BLOCK), :])

    loop(new_ref.shape[0], body)


def edge_forward_kernel(
    verts,
    count_ref,
    ends_ref,
    halo0_ref,
    halo1_ref,
    edges_ref,
    part_ref,
    far_ref,
    ef_ref,
    es_ref,
    pre_ref,
    hidden_ref,
    normed_ref,
    inv_ref,
    new_ref,
    back0_ref,
    back1_ref,
    seam_ref,
):
    features = edges_ref.shape[1]
    slots = halo0_ref.shape[0]
    count = count_ref[0]
    halo = jnp.concatenate([halo0_ref[...], halo1_ref[...]], axis=0)
    seam_ref[...] = jnp.zeros_like(seam_ref)

    def body(start):
        rows = pl.ds(start, BLOCK)
        far_rows = dot(far_ref[rows, :], halo).astype(BF)
        pre = part_ref[rows, :] + dot(far_rows, ef_ref[2 * features :, :])
        pre_ref[rows, :] = pre
        hidden = (pre * sigmoid(pre)).astype(BF)
        hidden_ref[rows, :] = hidden
        normed, inv = normalize(dot(hidden, es_ref[...]))
        normed_ref[rows, :] = normed
        inv_ref[rows, :] = inv
        new_edge = (edges_ref[rows, :].astype(F32) + normed).astype(BF)
        new_ref[rows, :] = new_edge
        second = live_row(ends_ref, 1, start, count)
        away = one_hot(second - verts, (2 * slots, BLOCK), 0).astype(BF)
        seam_ref[...] += dot(away, new_edge)

    loop(edges_ref.shape[0], body)
    back0_ref[...] = seam_ref[:slots, :]
    back1_ref[...] = seam_ref[slots:, :]


def node_kernel(
    pick_ref,
    spread_ref,
    nodes_ref,
    cot_ref,
    agg_ref,
    got0_ref,
    got1_ref,
    nf_ref,
    ns_ref,
    new_ref,
    agg16_ref,
    hidden_ref,
    dout_ref,
    dpre_ref,
    dagg_ref,
    out0_ref,
    out1_ref,
):
    verts, features = nodes_ref.shape
    got = jnp.concatenate([got0_ref[...], got1_ref[...]], axis=0)
    aggregate = (agg_ref[...] + seam_spread(spread_ref, got)).astype(BF)
    agg16_ref[...] = aggregate
    node_rows = nodes_ref[...]
    pre = dot(node_rows, nf_ref[:features, :]) + dot(aggregate, nf_ref[features:, :])
    sigma = sigmoid(pre)
    hidden = (pre * sigma).astype(BF)
    hidden_ref[...] = hidden
    normed, inv = normalize(dot(hidden, ns_ref[...]))
    new_ref[...] = (node_rows.astype(F32) + normed).astype(BF)
    d_out = norm_back(cot_ref[...].astype(F32), normed, inv).astype(BF)
    dout_ref[...] = d_out
    d_pre = (dot_t(d_out, ns_ref[...]) * (sigma * (1.0 + pre * (1.0 - sigma)))).astype(BF)
    dpre_ref[...] = d_pre
    d_agg = dot_t(d_pre, nf_ref[features:, :]).astype(BF)
    dagg_ref[...] = d_agg
    picked = dot(pick_ref[...], d_agg).astype(BF)
    slots = out0_ref.shape[0]
    out0_ref[...] = picked[:slots]
    out1_ref[...] = picked[slots:]


def fill_kernel(
    nodes_ref,
    cot_ref,
    agg16_ref,
    hidden_ref,
    dout_ref,
    dpre_ref,
    dagg_ref,
    nf_ref,
    pairs_ref,
    grad_ref,
    part_ref,
    up_ref,
):
    features = nodes_ref.shape[1]
    d_pre = dpre_ref[...]

    def body(start):
        rows = pl.ds(start, BLOCK)
        up_ref[rows, :] = dot(pairs_ref[rows, :], dagg_ref[...])

    loop(pairs_ref.shape[0], body)
    grad_ref[:features, :] = t_dot(nodes_ref[...], d_pre).astype(BF)
    grad_ref[features : 2 * features, :] = t_dot(agg16_ref[...], d_pre).astype(BF)
    grad_ref[2 * features :, :] = t_dot(hidden_ref[...], dout_ref[...]).astype(BF)
    part_ref[...] = cot_ref[...].astype(F32) + dot_t(d_pre, nf_ref[:features, :])


def edge_backward_kernel(
    count_ref,
    ends_ref,
    nodes_ref,
    halo0_ref,
    halo1_ref,
    edges_ref,
    up_ref,
    far_ref,
    dhalo0_ref,
    dhalo1_ref,
    pre_ref,
    hidden_ref,
    normed_ref,
    inv_ref,
    ef_ref,
    es_ref,
    nodegrad_ref,
    part_ref,
    gedges_ref,
    pack_ref,
    partout_ref,
    back0_ref,
    back1_ref,
    first_ref,
    second_ref,
    seam_ref,
    ges_ref,
    ge1_ref,
):
    features = edges_ref.shape[1]
    half = features // 2
    verts = nodes_ref.shape[0]
    slots = halo0_ref.shape[0]
    count = count_ref[0]
    d_halo = jnp.concatenate([dhalo0_ref[...], dhalo1_ref[...]], axis=0)
    for ref in (first_ref, second_ref, seam_ref, ges_ref, ge1_ref):
        ref[...] = jnp.zeros_like(ref)

    def body(start):
        rows = pl.ds(start, BLOCK)
        up = up_ref[rows, :] + dot(far_ref[rows, :], d_halo)
        d_out = norm_back(up, normed_ref[rows, :], inv_ref[rows, :]).astype(BF)
        ges_ref[...] += t_dot(hidden_ref[rows, :], d_out)
        d_pre = (dot_t(d_out, es_ref[...]) * slope(pre_ref[rows, :])).astype(BF)
        first = live_row(ends_ref, 0, start, count)
        second = live_row(ends_ref, 1, start, count)
        seam_ref[...] += dot(one_hot(second - verts, (2 * slots, BLOCK), 0).astype(BF), d_pre)
        first_ref[...] += dot(one_hot(first, (verts, BLOCK), 0).astype(BF), d_pre)
        second_ref[...] += dot(one_hot(second, (verts, BLOCK), 0).astype(BF), d_pre)
        ge1_ref[...] += t_dot(edges_ref[rows, :], d_pre)
        gedges_ref[rows, :] = (up + dot_t(d_pre, ef_ref[:features, :])).astype(BF)

    loop(edges_ref.shape[0], body)
    back0_ref[...] = seam_ref[:slots, :]
    back1_ref[...] = seam_ref[slots:, :]
    total = pack_ref.shape[0] // 2

    def put(begin, grad):
        grad = grad.astype(BF)
        size = grad.shape[0]
        pack_ref[begin : begin + size, :] = grad[:, :half]
        pack_ref[total + begin : total + begin + size, :] = grad[:, half:]

    node_rows = nodes_ref[...]
    first = first_ref[...].astype(BF)
    second = second_ref[...].astype(BF)
    far = seam_ref[...].astype(BF)
    halo = jnp.concatenate([halo0_ref[...], halo1_ref[...]], axis=0)
    put(0, ge1_ref[...])
    put(features, t_dot(node_rows, first))
    put(
        2 * features,
        t_dot(node_rows, second) + t_dot(halo, far),
    )
    put(3 * features, ges_ref[...])
    put(4 * features, nodegrad_ref[...])
    middle = ef_ref[features : 2 * features, :]
    last = ef_ref[2 * features :, :]
    partout_ref[...] = (
        part_ref[...] + dot_t(first, middle) + dot_t(second, last)
    )


def finish_kernel(spread_ref, part_ref, got0_ref, got1_ref, ef_ref, out_ref):
    features = part_ref.shape[1]
    got = jnp.concatenate([got0_ref[...], got1_ref[...]], axis=0)
    high, low = split(got)
    last = ef_ref[2 * features :, :]
    ends = dot_t(high, last) + dot_t(low, last)
    out_ref[...] = (part_ref[...] + seam_spread(spread_ref, ends)).astype(BF)


def unpack_kernel(pack_ref, gef_ref, ges_ref, gnf_ref, gns_ref):
    total = pack_ref.shape[0] // 2
    half = pack_ref.shape[1]
    begin = 0
    for ref in (gef_ref, ges_ref, gnf_ref, gns_ref):
        size = ref.shape[0]
        ref[:, :half] = pack_ref[begin : begin + size, :]
        ref[:, half:] = pack_ref[total + begin : total + begin + size, :]
        begin += size


def call(kernel, outs, args, scalars=0, scratch=(), flops=0, name=None):
    return pl.pallas_call(
        kernel,
        out_shape=[jax.ShapeDtypeStruct(shape, kind) for shape, kind in outs],
        in_specs=[
            pl.BlockSpec(memory_space=pltpu.SMEM if i < scalars else pltpu.VMEM)
            for i in range(len(args))
        ],
        out_specs=[pl.BlockSpec(memory_space=pltpu.VMEM) for _ in outs],
        scratch_shapes=[pltpu.VMEM(shape, F32) for shape in scratch],
        compiler_params=pltpu.CompilerParams(vmem_limit_bytes=24 * 2**20),
        cost_estimate=pl.CostEstimate(flops=flops, transcendentals=0, bytes_accessed=flops // 1000),
        name=name,
    )(*args)


def shift(block, distance):
    count = lax.axis_size(PATCH)
    return lax.ppermute(block, PATCH, [((i - distance) % count, i) for i in range(count)])


def group_size(axes):
    return lax.axis_size(axes)


def sum_kernel(pieces_ref, side0_ref, side1_ref, out_ref, pass0_ref, pass1_ref):
    count = pieces_ref.shape[0]
    copies = out_ref.shape[0]
    pass0_ref[...] = side0_ref[...]
    pass1_ref[...] = side1_ref[...]
    total = lax.fori_loop(
        1,
        count,
        lambda i, acc: acc + pieces_ref[i].astype(F32),
        pieces_ref[0].astype(F32),
        unroll=7,
    ).astype(BF)

    def store(i, carry):
        out_ref[i] = total
        return carry

    lax.fori_loop(0, copies, store, 0, unroll=8)


def sum_and_copy(pieces, side0, side1, copies, name):
    return call(
        sum_kernel,
        [
            ((copies,) + pieces.shape[1:], BF),
            (side0.shape, side0.dtype),
            (side1.shape, side1.dtype),
        ],
        (pieces, side0, side1),
        flops=pieces.size,
        name=name,
    )


def sum_everywhere(pack, back0, back1):
    inner = group_size(INNER)
    outer = group_size(OUTER)
    rows, lanes = pack.shape
    pieces = lax.all_to_all(pack.reshape(inner, rows // inner, lanes), INNER, 0, 0)
    pieces, back0, back1 = sum_and_copy(pieces, back0, back1, outer, "inner_sum")
    pieces = lax.all_to_all(pieces, OUTER, 0, 0)
    got0 = shift(back0, 1)
    got1 = shift(back1, 2)
    pieces, got0, got1 = sum_and_copy(pieces, got0, got1, inner, "outer_sum")
    pieces = lax.all_to_all(pieces, INNER, 0, 0)
    return pieces.reshape(rows, lanes), got0, got1


def local(
    nodes,
    edges,
    edge_ends,
    edge_count,
    send_rows,
    cotangent,
    edge_first,
    edge_second,
    node_first,
    node_second,
):
    node_rows = nodes[0]
    edge_rows = edges[0]
    cot = cotangent[0]
    verts, features = node_rows.shape
    slots = edge_rows.shape[0]
    hops, seam = send_rows.shape
    assert hops == 2
    ends = edge_ends.T
    seam16 = ((seam, features), BF)
    seam32 = ((seam, features), F32)
    unit = 2 * features * features

    out0, out1, node_rows, ends, edge_first, edge_rows, pick, spread = load(
        (send_rows, node_rows, ends, edge_first, edge_rows)
    )
    halo0 = shift(out0, -1)
    halo1 = shift(out1, -2)
    part, pairs, far = call(
        edge_local_kernel,
        [((slots, features), F32), ((slots, verts), BF), ((slots, hops * seam), BF)],
        (edge_count, ends, node_rows, edge_rows, edge_first),
        scalars=1,
        flops=7 * slots * unit,
        name="edge_local",
    )
    pre, hidden, normed, inv, new_edge, back0, back1 = call(
        functools.partial(edge_forward_kernel, verts),
        [
            ((slots, features), F32),
            ((slots, features), BF),
            ((slots, features), F32),
            ((slots, 1), F32),
            ((slots, features), BF),
            seam32,
            seam32,
        ],
        (edge_count, ends, halo0, halo1, edge_rows, part, far, edge_first, edge_second),
        scalars=1,
        scratch=[(hops * seam, features)],
        flops=4 * slots * unit,
        name="edge_forward",
    )
    got0 = shift(back0, 1)
    got1 = shift(back1, 2)
    tall = (verts, features)
    (agg,) = call(
        aggregate_kernel,
        [(tall, F32)],
        (edge_count, ends, new_edge),
        scalars=1,
        flops=4 * slots * unit,
        name="aggregate",
    )
    new_nodes, agg16, node_hidden, d_out, d_pre, d_agg, out0, out1 = call(
        node_kernel,
        [(tall, BF)] * 6 + [seam16, seam16],
        (pick, spread, node_rows, cot, agg, got0, got1, node_first, node_second),
        flops=8 * verts * unit,
        name="node",
    )
    d_halo0 = shift(out0, -1)
    d_halo1 = shift(out1, -2)
    node_grads, grad_part, up = call(
        fill_kernel,
        [((3 * features, features), BF), (tall, F32), ((slots, features), F32)],
        (node_rows, cot, agg16, node_hidden, d_out, d_pre, d_agg, node_first, pairs),
        flops=4 * slots * unit,
        name="fill",
    )
    grad_edges, pack, grad_part, back0, back1 = call(
        edge_backward_kernel,
        [
            ((slots, features), BF),
            ((2 * 7 * features, features // 2), BF),
            (tall, F32),
            seam32,
            seam32,
        ],
        (
            edge_count,
            ends,
            node_rows,
            halo0,
            halo1,
            edge_rows,
            up,
            far,
            d_halo0,
            d_halo1,
            pre,
            hidden,
            normed,
            inv,
            edge_first,
            edge_second,
            node_grads,
            grad_part,
        ),
        scalars=1,
        scratch=[tall, tall, (hops * seam, features), (features, features), (features, features)],
        flops=12 * slots * unit,
        name="edge_backward",
    )
    pack, got0, got1 = sum_everywhere(pack, back0, back1)
    (grad_nodes,) = call(
        finish_kernel,
        [(tall, BF)],
        (spread, grad_part, got0, got1, edge_first),
        flops=verts * unit,
        name="finish",
    )
    grad_ef, grad_es, grad_nf, grad_ns = call(
        unpack_kernel,
        [
            ((3 * features, features), BF),
            ((features, features), BF),
            ((2 * features, features), BF),
            ((features, features), BF),
        ],
        (pack,),
        flops=1000,
        name="unpack",
    )
    return (
        new_nodes[None],
        grad_nodes[None],
        grad_edges[None],
        grad_ef,
        grad_es,
        grad_nf,
        grad_ns,
    )


def solution(mesh):
    fine = Mesh(mesh.devices.reshape(PATCH_SPLIT + (mesh.shape["rep"],)), PATCH + ("rep",))
    placed = (
        P("rep", PATCH, None),
        P("rep", PATCH, None),
        P(PATCH, None),
        P(PATCH),
        P(PATCH, None),
        P("rep", PATCH, None),
        P(),
        P(),
        P(),
        P(),
    )
    return jax.shard_map(
        local,
        mesh=fine,
        in_specs=placed,
        out_specs=(
            P("rep", PATCH, None),
            P("rep", PATCH, None),
            P("rep", PATCH, None),
            P(),
            P(),
            P(),
            P(),
        ),
        check_vma=False,
    )
```

```python
import functools

import jax
import jax.numpy as jnp
from jax import lax
from jax.experimental import pallas as pl
from jax.experimental.pallas import tpu as pltpu
from jax.sharding import Mesh, PartitionSpec as P

EPS = 1e-05
BF = jnp.bfloat16
F32 = jnp.float32
BLOCK = 1536
PATCH_SPLIT = (4, 8, 2, 2)
PATCH = ("y", "zh", "zl", "c")
INNER = ("y", "zl", "rep")
OUTER = ("zh",)


def dot(left, right):
    return jnp.dot(left, right, preferred_element_type=F32)


def dot_t(left, right):
    return lax.dot_general(left, right, (((1,), (1,)), ((), ())), preferred_element_type=F32)


def t_dot(left, right):
    return lax.dot_general(left, right, (((0,), (0,)), ((), ())), preferred_element_type=F32)


def split(values):
    high = values.astype(BF)
    return high, (values - high.astype(F32)).astype(BF)


def one_hot(index, shape, axis):
    return (index == lax.broadcasted_iota(jnp.int32, shape, axis)).astype(F32)


def normalize(values):
    centred = values - jnp.mean(values, axis=-1, keepdims=True)
    inv_scale = lax.rsqrt(jnp.mean(centred * centred, axis=-1, keepdims=True) + EPS)
    return centred * inv_scale, inv_scale


def norm_back(upstream, normed, inv_scale):
    return inv_scale * (
        upstream
        - jnp.mean(upstream, axis=-1, keepdims=True)
        - normed * jnp.mean(upstream * normed, axis=-1, keepdims=True)
    )


def sigmoid(pre):
    return 1.0 / (1.0 + jnp.exp(-pre))


def slope(pre):
    sigma = sigmoid(pre)
    return sigma * (1.0 + pre * (1.0 - sigma))


def live_row(ends_ref, row, start, count, offset=0):
    index = ends_ref[row : row + 1, pl.ds(start, BLOCK)]
    slot = start + lax.broadcasted_iota(jnp.int32, (1, BLOCK), 1)
    return jnp.where(slot < count, index - offset, -1)


def loop(total, body):
    def step(i, carry):
        body(pl.multiple_of(i * BLOCK, BLOCK))
        return carry

    lax.fori_loop(0, total // BLOCK, step, 0)


def seam_tables(send_ref, pick_ref, spread_ref):
    hops, slots = send_ref.shape
    wide, verts = pick_ref.shape
    flat = jnp.concatenate([send_ref[hop : hop + 1, :] for hop in range(hops)], axis=1)
    spread = one_hot(flat, (verts, wide), 0)
    spread_ref[...] = jnp.concatenate([spread, spread], axis=1).astype(BF)
    column = jnp.broadcast_to(flat, (8, wide)).T[:, 0:1]
    pick_ref[...] = one_hot(column, (wide, verts), 1).astype(BF)


def seam_spread(spread_ref, rows):
    high, low = split(rows)
    return dot(spread_ref[...], jnp.concatenate([high, low], axis=0))


def load_kernel(
    send_hbm,
    nodes_hbm,
    ends_hbm,
    ef_hbm,
    edges_hbm,
    out0_ref,
    out1_ref,
    nodes_ref,
    ends_ref,
    ef_ref,
    edges_ref,
    pick_ref,
    spread_ref,
    send_ref,
    sems,
):
    sources = (send_hbm, nodes_hbm, ends_hbm, ef_hbm, edges_hbm)
    targets = (send_ref, nodes_ref, ends_ref, ef_ref, edges_ref)
    copies = [
        pltpu.make_async_copy(source, target, sems.at[i])
        for i, (source, target) in enumerate(zip(sources, targets))
    ]
    for copy in copies:
        copy.start()
    copies[0].wait()
    seam_tables(send_ref, pick_ref, spread_ref)
    copies[1].wait()
    picked = dot(pick_ref[...], nodes_ref[...]).astype(BF)
    slots = out0_ref.shape[0]
    out0_ref[...] = picked[:slots]
    out1_ref[...] = picked[slots:]
    for copy in copies[2:]:
        copy.wait()


def load(sources):
    send, nodes = sources[:2]
    wide = send.shape[0] * send.shape[1]
    outs = [jax.ShapeDtypeStruct(x.shape, x.dtype) for x in sources[1:]]
    outs.append(jax.ShapeDtypeStruct((wide, nodes.shape[0]), BF))
    outs.append(jax.ShapeDtypeStruct((nodes.shape[0], 2 * wide), BF))
    seam = jax.ShapeDtypeStruct((send.shape[1], nodes.shape[1]), BF)
    return pl.pallas_call(
        load_kernel,
        out_shape=[seam, seam] + outs,
        in_specs=[pl.BlockSpec(memory_space=pltpu.HBM) for _ in sources],
        out_specs=[pl.BlockSpec(memory_space=pltpu.VMEM) for _ in range(2 + len(outs))],
        scratch_shapes=[
            pltpu.VMEM(send.shape, send.dtype),
            pltpu.SemaphoreType.DMA((len(sources),)),
        ],
        compiler_params=pltpu.CompilerParams(vmem_limit_bytes=24 * 2**20),
        cost_estimate=pl.CostEstimate(flops=10**8, transcendentals=0, bytes_accessed=10**6),
        name="load",
    )(*[pltpu.with_memory_space_constraint(x, pltpu.HBM) for x in sources])


def edge_local_kernel(
    count_ref, ends_ref, nodes_ref, edges_ref, ef_ref, pre_ref, pairs_ref, far_ref
):
    features = nodes_ref.shape[1]
    verts = nodes_ref.shape[0]
    seam = far_ref.shape[1]
    count = count_ref[0]

    def body(start):
        rows = pl.ds(start, BLOCK)
        first = live_row(ends_ref, 0, start, count)
        second = live_row(ends_ref, 1, start, count)
        both = jnp.concatenate([first, second, second, second, second, second, second, second], axis=0)
        cols = both.T
        first_col = cols[:, 0:1]
        second_col = cols[:, 1:2]
        pick_first = one_hot(first_col, (BLOCK, verts), 1)
        pick_second = one_hot(second_col, (BLOCK, verts), 1)
        far_ref[rows, :] = one_hot(second_col - verts, (BLOCK, seam), 1).astype(BF)
        pairs_ref[rows, :] = (pick_first + pick_second).astype(BF)
        table = nodes_ref[...]
        first_rows = dot(pick_first.astype(BF), table).astype(BF)
        second_rows = dot(pick_second.astype(BF), table).astype(BF)
        pre_ref[rows, :] = (
            dot(edges_ref[rows, :], ef_ref[:features, :])
            + dot(first_rows, ef_ref[features : 2 * features, :])
            + dot(second_rows, ef_ref[2 * features :, :])
        )

    loop(edges_ref.shape[0], body)


def aggregate_kernel(count_ref, ends_ref, new_ref, agg_ref):
    verts = agg_ref.shape[0]
    count = count_ref[0]
    agg_ref[...] = jnp.zeros_like(agg_ref)

    def body(start):
        first = live_row(ends_ref, 0, start, count)
        second = live_row(ends_ref, 1, start, count)
        spread = one_hot(first, (verts, BLOCK), 0) + one_hot(second, (verts, BLOCK), 0)
        agg_ref[...] += dot(spread.astype(BF), new_ref[pl.ds(start, BLOCK), :])

    loop(new_ref.shape[0], body)


def edge_forward_kernel(
    verts,
    count_ref,
    ends_ref,
    halo0_ref,
    halo1_ref,
    edges_ref,
    part_ref,
    far_ref,
    ef_ref,
    es_ref,
    pre_ref,
    hidden_ref,
    normed_ref,
    inv_ref,
    new_ref,
    back0_ref,
    back1_ref,
    seam_ref,
):
    features = edges_ref.shape[1]
    slots = halo0_ref.shape[0]
    count = count_ref[0]
    halo = jnp.concatenate([halo0_ref[...], halo1_ref[...]], axis=0)
    seam_ref[...] = jnp.zeros_like(seam_ref)

    def body(start):
        rows = pl.ds(start, BLOCK)
        far_rows = dot(far_ref[rows, :], halo).astype(BF)
        pre = part_ref[rows, :] + dot(far_rows, ef_ref[2 * features :, :])
        pre_ref[rows, :] = pre
        hidden = (pre * sigmoid(pre)).astype(BF)
        hidden_ref[rows, :] = hidden
        normed, inv = normalize(dot(hidden, es_ref[...]))
        normed_ref[rows, :] = normed
        inv_ref[rows, :] = inv
        new_edge = (edges_ref[rows, :].astype(F32) + normed).astype(BF)
        new_ref[rows, :] = new_edge
        second = live_row(ends_ref, 1, start, count)
        away = one_hot(second - verts, (2 * slots, BLOCK), 0).astype(BF)
        seam_ref[...] += dot(away, new_edge)

    loop(edges_ref.shape[0], body)
    back0_ref[...] = seam_ref[:slots, :]
    back1_ref[...] = seam_ref[slots:, :]


def node_kernel(
    pick_ref,
    spread_ref,
    nodes_ref,
    cot_ref,
    agg_ref,
    got0_ref,
    got1_ref,
    nf_ref,
    ns_ref,
    new_ref,
    agg16_ref,
    hidden_ref,
    dout_ref,
    dpre_ref,
    dagg_ref,
    out0_ref,
    out1_ref,
):
    verts, features = nodes_ref.shape
    got = jnp.concatenate([got0_ref[...], got1_ref[...]], axis=0)
    aggregate = (agg_ref[...] + seam_spread(spread_ref, got)).astype(BF)
    agg16_ref[...] = aggregate
    node_rows = nodes_ref[...]
    pre = dot(node_rows, nf_ref[:features, :]) + dot(aggregate, nf_ref[features:, :])
    sigma = sigmoid(pre)
    hidden = (pre * sigma).astype(BF)
    hidden_ref[...] = hidden
    normed, inv = normalize(dot(hidden, ns_ref[...]))
    new_ref[...] = (node_rows.astype(F32) + normed).astype(BF)
    d_out = norm_back(cot_ref[...].astype(F32), normed, inv).astype(BF)
    dout_ref[...] = d_out
    d_pre = (dot_t(d_out, ns_ref[...]) * (sigma * (1.0 + pre * (1.0 - sigma)))).astype(BF)
    dpre_ref[...] = d_pre
    d_agg = dot_t(d_pre, nf_ref[features:, :]).astype(BF)
    dagg_ref[...] = d_agg
    picked = dot(pick_ref[...], d_agg).astype(BF)
    slots = out0_ref.shape[0]
    out0_ref[...] = picked[:slots]
    out1_ref[...] = picked[slots:]


def fill_kernel(
    nodes_ref,
    cot_ref,
    agg16_ref,
    hidden_ref,
    dout_ref,
    dpre_ref,
    dagg_ref,
    nf_ref,
    pairs_ref,
    grad_ref,
    part_ref,
    up_ref,
):
    features = nodes_ref.shape[1]
    d_pre = dpre_ref[...]

    def body(start):
        rows = pl.ds(start, BLOCK)
        up_ref[rows, :] = dot(pairs_ref[rows, :], dagg_ref[...])

    loop(pairs_ref.shape[0], body)
    grad_ref[:features, :] = t_dot(nodes_ref[...], d_pre).astype(BF)
    grad_ref[features : 2 * features, :] = t_dot(agg16_ref[...], d_pre).astype(BF)
    grad_ref[2 * features :, :] = t_dot(hidden_ref[...], dout_ref[...]).astype(BF)
    part_ref[...] = cot_ref[...].astype(F32) + dot_t(d_pre, nf_ref[:features, :])


def edge_backward_kernel(
    count_ref,
    core_ref,
    ends_ref,
    nodes_ref,
    halo0_ref,
    halo1_ref,
    edges_ref,
    up_ref,
    far_ref,
    dhalo0_ref,
    dhalo1_ref,
    pre_ref,
    hidden_ref,
    normed_ref,
    inv_ref,
    ef_ref,
    es_ref,
    nodegrad_ref,
    part_ref,
    gedges_ref,
    keep_ref,
    give_ref,
    partout_ref,
    back0_ref,
    back1_ref,
    first_ref,
    second_ref,
    seam_ref,
    ges_ref,
    ge1_ref,
):
    features = edges_ref.shape[1]
    verts = nodes_ref.shape[0]
    slots = halo0_ref.shape[0]
    count = count_ref[0]
    d_halo = jnp.concatenate([dhalo0_ref[...], dhalo1_ref[...]], axis=0)
    for ref in (first_ref, second_ref, seam_ref, ges_ref, ge1_ref):
        ref[...] = jnp.zeros_like(ref)

    def body(start):
        rows = pl.ds(start, BLOCK)
        up = up_ref[rows, :] + dot(far_ref[rows, :], d_halo)
        d_out = norm_back(up, normed_ref[rows, :], inv_ref[rows, :]).astype(BF)
        ges_ref[...] += t_dot(hidden_ref[rows, :], d_out)
        d_pre = (dot_t(d_out, es_ref[...]) * slope(pre_ref[rows, :])).astype(BF)
        first = live_row(ends_ref, 0, start, count)
        second = live_row(ends_ref, 1, start, count)
        seam_ref[...] += dot(one_hot(second - verts, (2 * slots, BLOCK), 0).astype(BF), d_pre)
        first_ref[...] += dot(one_hot(first, (verts, BLOCK), 0).astype(BF), d_pre)
        second_ref[...] += dot(one_hot(second, (verts, BLOCK), 0).astype(BF), d_pre)
        ge1_ref[...] += t_dot(edges_ref[rows, :], d_pre)
        gedges_ref[rows, :] = (up + dot_t(d_pre, ef_ref[:features, :])).astype(BF)

    loop(edges_ref.shape[0], body)
    back0_ref[...] = seam_ref[:slots, :]
    back1_ref[...] = seam_ref[slots:, :]
    half = features // 2
    low_core = core_ref[0] == 0

    def put(begin, grad):
        grad = grad.astype(BF)
        size = grad.shape[0]
        left = grad[:, :half]
        right = grad[:, half:]
        keep_ref[begin : begin + size, :] = jnp.where(low_core, left, right)
        give_ref[begin : begin + size, :] = jnp.where(low_core, right, left)

    node_rows = nodes_ref[...]
    first = first_ref[...].astype(BF)
    second = second_ref[...].astype(BF)
    far = seam_ref[...].astype(BF)
    halo = jnp.concatenate([halo0_ref[...], halo1_ref[...]], axis=0)
    put(0, ge1_ref[...])
    put(features, t_dot(node_rows, first))
    put(
        2 * features,
        t_dot(node_rows, second) + t_dot(halo, far),
    )
    put(3 * features, ges_ref[...])
    put(4 * features, nodegrad_ref[...])
    middle = ef_ref[features : 2 * features, :]
    last = ef_ref[2 * features :, :]
    partout_ref[...] = (
        part_ref[...] + dot_t(first, middle) + dot_t(second, last)
    )


def finish_kernel(spread_ref, part_ref, got0_ref, got1_ref, ef_ref, out_ref):
    features = part_ref.shape[1]
    got = jnp.concatenate([got0_ref[...], got1_ref[...]], axis=0)
    high, low = split(got)
    last = ef_ref[2 * features :, :]
    ends = dot_t(high, last) + dot_t(low, last)
    out_ref[...] = (part_ref[...] + seam_spread(spread_ref, ends)).astype(BF)


def unpack_kernel(core_ref, mine_ref, other_ref, gef_ref, ges_ref, gnf_ref, gns_ref):
    half = mine_ref.shape[1]
    low_core = core_ref[0] == 0
    begin = 0
    for ref in (gef_ref, ges_ref, gnf_ref, gns_ref):
        size = ref.shape[0]
        mine = mine_ref[begin : begin + size, :]
        other = other_ref[begin : begin + size, :]
        ref[:, :half] = jnp.where(low_core, mine, other)
        ref[:, half:] = jnp.where(low_core, other, mine)
        begin += size


def call(kernel, outs, args, scalars=0, scratch=(), flops=0, name=None):
    return pl.pallas_call(
        kernel,
        out_shape=[jax.ShapeDtypeStruct(shape, kind) for shape, kind in outs],
        in_specs=[
            pl.BlockSpec(memory_space=pltpu.SMEM if i < scalars else pltpu.VMEM)
            for i in range(len(args))
        ],
        out_specs=[pl.BlockSpec(memory_space=pltpu.VMEM) for _ in outs],
        scratch_shapes=[pltpu.VMEM(shape, F32) for shape in scratch],
        compiler_params=pltpu.CompilerParams(vmem_limit_bytes=24 * 2**20),
        cost_estimate=pl.CostEstimate(flops=flops, transcendentals=0, bytes_accessed=flops // 1000),
        name=name,
    )(*args)


def shift(block, distance):
    count = lax.axis_size(PATCH)
    return lax.ppermute(block, PATCH, [((i - distance) % count, i) for i in range(count)])


def group_size(axes):
    return lax.axis_size(axes)


def sum_kernel(pieces_ref, side0_ref, side1_ref, out_ref, pass0_ref, pass1_ref):
    count = pieces_ref.shape[0]
    copies = out_ref.shape[0]
    pass0_ref[...] = side0_ref[...]
    pass1_ref[...] = side1_ref[...]
    total = lax.fori_loop(
        1,
        count,
        lambda i, acc: acc + pieces_ref[i].astype(F32),
        pieces_ref[0].astype(F32),
        unroll=7,
    ).astype(BF)

    def store(i, carry):
        out_ref[i] = total
        return carry

    lax.fori_loop(0, copies, store, 0, unroll=8)


def sum_and_copy(pieces, side0, side1, copies, name):
    return call(
        sum_kernel,
        [
            ((copies,) + pieces.shape[1:], BF),
            (side0.shape, side0.dtype),
            (side1.shape, side1.dtype),
        ],
        (pieces, side0, side1),
        flops=pieces.size,
        name=name,
    )


def add_kernel(keep_ref, got_ref, out_ref):
    out_ref[...] = (keep_ref[...].astype(F32) + got_ref[...].astype(F32)).astype(BF)


def swap_cores(block):
    count = lax.axis_size("c")
    return lax.ppermute(block, "c", [((i + 1) % count, i) for i in range(count)])


def sum_everywhere(keep, give, back0, back1):
    inner = group_size(INNER)
    outer = group_size(OUTER)
    rows, lanes = keep.shape
    (pair,) = call(
        add_kernel, [(keep.shape, BF)], (keep, swap_cores(give)), flops=keep.size, name="core_sum"
    )
    pieces = lax.all_to_all(pair.reshape(inner, rows // inner, lanes), INNER, 0, 0)
    pieces, back0, back1 = sum_and_copy(pieces, back0, back1, outer, "inner_sum")
    pieces = lax.all_to_all(pieces, OUTER, 0, 0)
    got0 = shift(back0, 1)
    got1 = shift(back1, 2)
    pieces, got0, got1 = sum_and_copy(pieces, got0, got1, inner, "outer_sum")
    mine = lax.all_to_all(pieces, INNER, 0, 0).reshape(rows, lanes)
    return mine, swap_cores(mine), got0, got1


def local(
    nodes,
    edges,
    edge_ends,
    edge_count,
    send_rows,
    cotangent,
    edge_first,
    edge_second,
    node_first,
    node_second,
):
    node_rows = nodes[0]
    edge_rows = edges[0]
    cot = cotangent[0]
    verts, features = node_rows.shape
    slots = edge_rows.shape[0]
    hops, seam = send_rows.shape
    assert hops == 2
    ends = edge_ends.T
    core = lax.axis_index("c").astype(jnp.int32).reshape(1)
    seam16 = ((seam, features), BF)
    seam32 = ((seam, features), F32)
    unit = 2 * features * features

    out0, out1, node_rows, ends, edge_first, edge_rows, pick, spread = load(
        (send_rows, node_rows, ends, edge_first, edge_rows)
    )
    halo0 = shift(out0, -1)
    halo1 = shift(out1, -2)
    part, pairs, far = call(
        edge_local_kernel,
        [((slots, features), F32), ((slots, verts), BF), ((slots, hops * seam), BF)],
        (edge_count, ends, node_rows, edge_rows, edge_first),
        scalars=1,
        flops=7 * slots * unit,
        name="edge_local",
    )
    pre, hidden, normed, inv, new_edge, back0, back1 = call(
        functools.partial(edge_forward_kernel, verts),
        [
            ((slots, features), F32),
            ((slots, features), BF),
            ((slots, features), F32),
            ((slots, 1), F32),
            ((slots, features), BF),
            seam32,
            seam32,
        ],
        (edge_count, ends, halo0, halo1, edge_rows, part, far, edge_first, edge_second),
        scalars=1,
        scratch=[(hops * seam, features)],
        flops=4 * slots * unit,
        name="edge_forward",
    )
    got0 = shift(back0, 1)
    got1 = shift(back1, 2)
    tall = (verts, features)
    (agg,) = call(
        aggregate_kernel,
        [(tall, F32)],
        (edge_count, ends, new_edge),
        scalars=1,
        flops=4 * slots * unit,
        name="aggregate",
    )
    new_nodes, agg16, node_hidden, d_out, d_pre, d_agg, out0, out1 = call(
        node_kernel,
        [(tall, BF)] * 6 + [seam16, seam16],
        (pick, spread, node_rows, cot, agg, got0, got1, node_first, node_second),
        flops=8 * verts * unit,
        name="node",
    )
    d_halo0 = shift(out0, -1)
    d_halo1 = shift(out1, -2)
    node_grads, grad_part, up = call(
        fill_kernel,
        [((3 * features, features), BF), (tall, F32), ((slots, features), F32)],
        (node_rows, cot, agg16, node_hidden, d_out, d_pre, d_agg, node_first, pairs),
        flops=4 * slots * unit,
        name="fill",
    )
    grad_edges, keep, give, grad_part, back0, back1 = call(
        edge_backward_kernel,
        [
            ((slots, features), BF),
            ((7 * features, features // 2), BF),
            ((7 * features, features // 2), BF),
            (tall, F32),
            seam32,
            seam32,
        ],
        (
            edge_count,
            core,
            ends,
            node_rows,
            halo0,
            halo1,
            edge_rows,
            up,
            far,
            d_halo0,
            d_halo1,
            pre,
            hidden,
            normed,
            inv,
            edge_first,
            edge_second,
            node_grads,
            grad_part,
        ),
        scalars=2,
        scratch=[tall, tall, (hops * seam, features), (features, features), (features, features)],
        flops=12 * slots * unit,
        name="edge_backward",
    )
    mine, other, got0, got1 = sum_everywhere(keep, give, back0, back1)
    (grad_nodes,) = call(
        finish_kernel,
        [(tall, BF)],
        (spread, grad_part, got0, got1, edge_first),
        flops=verts * unit,
        name="finish",
    )
    grad_ef, grad_es, grad_nf, grad_ns = call(
        unpack_kernel,
        [
            ((3 * features, features), BF),
            ((features, features), BF),
            ((2 * features, features), BF),
            ((features, features), BF),
        ],
        (core, mine, other),
        scalars=1,
        flops=1000,
        name="unpack",
    )
    return (
        new_nodes[None],
        grad_nodes[None],
        grad_edges[None],
        grad_ef,
        grad_es,
        grad_nf,
        grad_ns,
    )


def solution(mesh):
    fine = Mesh(mesh.devices.reshape(PATCH_SPLIT + (mesh.shape["rep"],)), PATCH + ("rep",))
    placed = (
        P("rep", PATCH, None),
        P("rep", PATCH, None),
        P(PATCH, None),
        P(PATCH),
        P(PATCH, None),
        P("rep", PATCH, None),
        P(),
        P(),
        P(),
        P(),
    )
    return jax.shard_map(
        local,
        mesh=fine,
        in_specs=placed,
        out_specs=(
            P("rep", PATCH, None),
            P("rep", PATCH, None),
            P("rep", PATCH, None),
            P(),
            P(),
            P(),
            P(),
        ),
        check_vma=False,
    )
```

```python
import functools

import jax
import jax.numpy as jnp
from jax import lax
from jax.experimental import pallas as pl
from jax.experimental.pallas import tpu as pltpu
from jax.sharding import Mesh, PartitionSpec as P

EPS = 1e-05
BF = jnp.bfloat16
F32 = jnp.float32
BLOCK = 1536
PATCH_SPLIT = (4, 8, 2, 2)
PATCH = ("y", "zh", "zl", "c")
INNER = ("y", "zl", "rep")
OUTER = ("zh",)


def dot(left, right):
    return jnp.dot(left, right, preferred_element_type=F32)


def dot_t(left, right):
    return lax.dot_general(left, right, (((1,), (1,)), ((), ())), preferred_element_type=F32)


def t_dot(left, right):
    return lax.dot_general(left, right, (((0,), (0,)), ((), ())), preferred_element_type=F32)


def split(values):
    high = values.astype(BF)
    return high, (values - high.astype(F32)).astype(BF)


def one_hot(index, shape, axis):
    return (index == lax.broadcasted_iota(jnp.int32, shape, axis)).astype(F32)


def normalize(values):
    centred = values - jnp.mean(values, axis=-1, keepdims=True)
    inv_scale = lax.rsqrt(jnp.mean(centred * centred, axis=-1, keepdims=True) + EPS)
    return centred * inv_scale, inv_scale


def norm_back(upstream, normed, inv_scale):
    return inv_scale * (
        upstream
        - jnp.mean(upstream, axis=-1, keepdims=True)
        - normed * jnp.mean(upstream * normed, axis=-1, keepdims=True)
    )


def sigmoid(pre):
    return 1.0 / (1.0 + jnp.exp(-pre))


def slope(pre):
    sigma = sigmoid(pre)
    return sigma * (1.0 + pre * (1.0 - sigma))


def live_row(ends_ref, row, start, count, offset=0):
    index = ends_ref[row : row + 1, pl.ds(start, BLOCK)]
    slot = start + lax.broadcasted_iota(jnp.int32, (1, BLOCK), 1)
    return jnp.where(slot < count, index - offset, -1)


def loop(total, body):
    def step(i, carry):
        body(pl.multiple_of(i * BLOCK, BLOCK))
        return carry

    lax.fori_loop(0, total // BLOCK, step, 0)


def seam_tables(send_ref, pick_ref, spread_ref):
    hops, slots = send_ref.shape
    wide, verts = pick_ref.shape
    flat = jnp.concatenate([send_ref[hop : hop + 1, :] for hop in range(hops)], axis=1)
    spread = one_hot(flat, (verts, wide), 0)
    spread_ref[...] = jnp.concatenate([spread, spread], axis=1).astype(BF)
    column = jnp.broadcast_to(flat, (8, wide)).T[:, 0:1]
    pick_ref[...] = one_hot(column, (wide, verts), 1).astype(BF)


def seam_spread(spread_ref, rows):
    high, low = split(rows)
    return dot(spread_ref[...], jnp.concatenate([high, low], axis=0))


def load_kernel(
    send_hbm,
    nodes_hbm,
    ends_hbm,
    ef_hbm,
    edges_hbm,
    out0_ref,
    out1_ref,
    nodes_ref,
    ends_ref,
    ef_ref,
    edges_ref,
    pick_ref,
    spread_ref,
    send_ref,
    sems,
):
    sources = (send_hbm, nodes_hbm, ends_hbm, ef_hbm, edges_hbm)
    targets = (send_ref, nodes_ref, ends_ref, ef_ref, edges_ref)
    copies = [
        pltpu.make_async_copy(source, target, sems.at[i])
        for i, (source, target) in enumerate(zip(sources, targets))
    ]
    for copy in copies:
        copy.start()
    copies[0].wait()
    seam_tables(send_ref, pick_ref, spread_ref)
    copies[1].wait()
    picked = dot(pick_ref[...], nodes_ref[...]).astype(BF)
    slots = out0_ref.shape[0]
    out0_ref[...] = picked[:slots]
    out1_ref[...] = picked[slots:]
    for copy in copies[2:]:
        copy.wait()


def load(sources):
    send, nodes = sources[:2]
    wide = send.shape[0] * send.shape[1]
    outs = [jax.ShapeDtypeStruct(x.shape, x.dtype) for x in sources[1:]]
    outs.append(jax.ShapeDtypeStruct((wide, nodes.shape[0]), BF))
    outs.append(jax.ShapeDtypeStruct((nodes.shape[0], 2 * wide), BF))
    seam = jax.ShapeDtypeStruct((send.shape[1], nodes.shape[1]), BF)
    return pl.pallas_call(
        load_kernel,
        out_shape=[seam, seam] + outs,
        in_specs=[pl.BlockSpec(memory_space=pltpu.HBM) for _ in sources],
        out_specs=[pl.BlockSpec(memory_space=pltpu.VMEM) for _ in range(2 + len(outs))],
        scratch_shapes=[
            pltpu.VMEM(send.shape, send.dtype),
            pltpu.SemaphoreType.DMA((len(sources),)),
        ],
        compiler_params=pltpu.CompilerParams(vmem_limit_bytes=24 * 2**20),
        cost_estimate=pl.CostEstimate(flops=10**8, transcendentals=0, bytes_accessed=10**6),
        name="load",
    )(*[pltpu.with_memory_space_constraint(x, pltpu.HBM) for x in sources])


def edge_local_kernel(
    count_ref, ends_ref, nodes_ref, edges_ref, ef_ref, pre_ref, pairs_ref, far_ref
):
    features = nodes_ref.shape[1]
    verts = nodes_ref.shape[0]
    seam = far_ref.shape[1]
    count = count_ref[0]

    def body(start):
        rows = pl.ds(start, BLOCK)
        first = live_row(ends_ref, 0, start, count)
        second = live_row(ends_ref, 1, start, count)
        both = jnp.concatenate([first, second, second, second, second, second, second, second], axis=0)
        cols = both.T
        first_col = cols[:, 0:1]
        second_col = cols[:, 1:2]
        pick_first = one_hot(first_col, (BLOCK, verts), 1)
        pick_second = one_hot(second_col, (BLOCK, verts), 1)
        far_ref[rows, :] = one_hot(second_col - verts, (BLOCK, seam), 1).astype(BF)
        pairs_ref[rows, :] = (pick_first + pick_second).astype(BF)
        table = nodes_ref[...]
        first_rows = dot(pick_first.astype(BF), table).astype(BF)
        second_rows = dot(pick_second.astype(BF), table).astype(BF)
        pre_ref[rows, :] = (
            dot(edges_ref[rows, :], ef_ref[:features, :])
            + dot(first_rows, ef_ref[features : 2 * features, :])
            + dot(second_rows, ef_ref[2 * features :, :])
        )

    loop(edges_ref.shape[0], body)


def aggregate_kernel(count_ref, ends_ref, new_ref, agg_ref):
    verts = agg_ref.shape[0]
    count = count_ref[0]
    agg_ref[...] = jnp.zeros_like(agg_ref)

    def body(start):
        first = live_row(ends_ref, 0, start, count)
        second = live_row(ends_ref, 1, start, count)
        spread = one_hot(first, (verts, BLOCK), 0) + one_hot(second, (verts, BLOCK), 0)
        agg_ref[...] += dot(spread.astype(BF), new_ref[pl.ds(start, BLOCK), :])

    loop(new_ref.shape[0], body)


def edge_forward_kernel(
    verts,
    count_ref,
    ends_ref,
    halo0_ref,
    halo1_ref,
    edges_ref,
    part_ref,
    far_ref,
    ef_ref,
    es_ref,
    pre_ref,
    hidden_ref,
    normed_ref,
    inv_ref,
    new_ref,
    back0_ref,
    back1_ref,
    seam_ref,
):
    features = edges_ref.shape[1]
    slots = halo0_ref.shape[0]
    count = count_ref[0]
    halo = jnp.concatenate([halo0_ref[...], halo1_ref[...]], axis=0)
    seam_ref[...] = jnp.zeros_like(seam_ref)

    def body(start):
        rows = pl.ds(start, BLOCK)
        far_rows = dot(far_ref[rows, :], halo).astype(BF)
        pre = part_ref[rows, :] + dot(far_rows, ef_ref[2 * features :, :])
        pre_ref[rows, :] = pre
        hidden = (pre * sigmoid(pre)).astype(BF)
        hidden_ref[rows, :] = hidden
        normed, inv = normalize(dot(hidden, es_ref[...]))
        normed_ref[rows, :] = normed
        inv_ref[rows, :] = inv
        new_edge = (edges_ref[rows, :].astype(F32) + normed).astype(BF)
        new_ref[rows, :] = new_edge
        second = live_row(ends_ref, 1, start, count)
        away = one_hot(second - verts, (2 * slots, BLOCK), 0).astype(BF)
        seam_ref[...] += dot(away, new_edge)

    loop(edges_ref.shape[0], body)
    back0_ref[...] = seam_ref[:slots, :]
    back1_ref[...] = seam_ref[slots:, :]


def node_kernel(
    pick_ref,
    spread_ref,
    nodes_ref,
    cot_ref,
    agg_ref,
    got0_ref,
    got1_ref,
    nf_ref,
    ns_ref,
    new_ref,
    agg16_ref,
    hidden_ref,
    dout_ref,
    dpre_ref,
    dagg_ref,
    out0_ref,
    out1_ref,
):
    verts, features = nodes_ref.shape
    got = jnp.concatenate([got0_ref[...], got1_ref[...]], axis=0)
    aggregate = (agg_ref[...] + seam_spread(spread_ref, got)).astype(BF)
    agg16_ref[...] = aggregate
    node_rows = nodes_ref[...]
    pre = dot(node_rows, nf_ref[:features, :]) + dot(aggregate, nf_ref[features:, :])
    sigma = sigmoid(pre)
    hidden = (pre * sigma).astype(BF)
    hidden_ref[...] = hidden
    normed, inv = normalize(dot(hidden, ns_ref[...]))
    new_ref[...] = (node_rows.astype(F32) + normed).astype(BF)
    d_out = norm_back(cot_ref[...].astype(F32), normed, inv).astype(BF)
    dout_ref[...] = d_out
    d_pre = (dot_t(d_out, ns_ref[...]) * (sigma * (1.0 + pre * (1.0 - sigma)))).astype(BF)
    dpre_ref[...] = d_pre
    d_agg = dot_t(d_pre, nf_ref[features:, :]).astype(BF)
    dagg_ref[...] = d_agg
    picked = dot(pick_ref[...], d_agg).astype(BF)
    slots = out0_ref.shape[0]
    out0_ref[...] = picked[:slots]
    out1_ref[...] = picked[slots:]


def fill_kernel(
    nodes_ref,
    cot_ref,
    agg16_ref,
    hidden_ref,
    dout_ref,
    dpre_ref,
    dagg_ref,
    nf_ref,
    pairs_ref,
    grad_ref,
    part_ref,
    up_ref,
):
    features = nodes_ref.shape[1]
    d_pre = dpre_ref[...]

    def body(start):
        rows = pl.ds(start, BLOCK)
        up_ref[rows, :] = dot(pairs_ref[rows, :], dagg_ref[...])

    loop(pairs_ref.shape[0], body)
    grad_ref[:features, :] = t_dot(nodes_ref[...], d_pre).astype(BF)
    grad_ref[features : 2 * features, :] = t_dot(agg16_ref[...], d_pre).astype(BF)
    grad_ref[2 * features :, :] = t_dot(hidden_ref[...], dout_ref[...]).astype(BF)
    part_ref[...] = cot_ref[...].astype(F32) + dot_t(d_pre, nf_ref[:features, :])


def edge_backward_kernel(
    count_ref,
    ends_ref,
    nodes_ref,
    halo0_ref,
    halo1_ref,
    edges_ref,
    up_ref,
    far_ref,
    dhalo0_ref,
    dhalo1_ref,
    pre_ref,
    hidden_ref,
    normed_ref,
    inv_ref,
    ef_ref,
    es_ref,
    nodegrad_ref,
    part_ref,
    gedges_ref,
    pack_ref,
    partout_ref,
    back0_ref,
    back1_ref,
    first_ref,
    second_ref,
    seam_ref,
    ges_ref,
    ge1_ref,
):
    features = edges_ref.shape[1]
    verts = nodes_ref.shape[0]
    slots = halo0_ref.shape[0]
    count = count_ref[0]
    d_halo = jnp.concatenate([dhalo0_ref[...], dhalo1_ref[...]], axis=0)
    for ref in (first_ref, second_ref, seam_ref, ges_ref, ge1_ref):
        ref[...] = jnp.zeros_like(ref)

    def body(start):
        rows = pl.ds(start, BLOCK)
        up = up_ref[rows, :] + dot(far_ref[rows, :], d_halo)
        d_out = norm_back(up, normed_ref[rows, :], inv_ref[rows, :]).astype(BF)
        ges_ref[...] += t_dot(hidden_ref[rows, :], d_out)
        d_pre = (dot_t(d_out, es_ref[...]) * slope(pre_ref[rows, :])).astype(BF)
        first = live_row(ends_ref, 0, start, count)
        second = live_row(ends_ref, 1, start, count)
        seam_ref[...] += dot(one_hot(second - verts, (2 * slots, BLOCK), 0).astype(BF), d_pre)
        first_ref[...] += dot(one_hot(first, (verts, BLOCK), 0).astype(BF), d_pre)
        second_ref[...] += dot(one_hot(second, (verts, BLOCK), 0).astype(BF), d_pre)
        ge1_ref[...] += t_dot(edges_ref[rows, :], d_pre)
        gedges_ref[rows, :] = (up + dot_t(d_pre, ef_ref[:features, :])).astype(BF)

    loop(edges_ref.shape[0], body)
    back0_ref[...] = seam_ref[:slots, :]
    back1_ref[...] = seam_ref[slots:, :]
    half = features // 2

    def put(begin, grad):
        grad = grad.astype(BF)
        size = grad.shape[0]
        left = grad[:, :half]
        right = grad[:, half:]
        pack_ref[0, begin : begin + size, :] = left
        pack_ref[1, begin : begin + size, :] = right

    node_rows = nodes_ref[...]
    first = first_ref[...].astype(BF)
    second = second_ref[...].astype(BF)
    far = seam_ref[...].astype(BF)
    halo = jnp.concatenate([halo0_ref[...], halo1_ref[...]], axis=0)
    put(0, ge1_ref[...])
    put(features, t_dot(node_rows, first))
    put(
        2 * features,
        t_dot(node_rows, second) + t_dot(halo, far),
    )
    put(3 * features, ges_ref[...])
    put(4 * features, nodegrad_ref[...])
    middle = ef_ref[features : 2 * features, :]
    last = ef_ref[2 * features :, :]
    partout_ref[...] = (
        part_ref[...] + dot_t(first, middle) + dot_t(second, last)
    )


def finish_kernel(spread_ref, part_ref, got0_ref, got1_ref, ef_ref, out_ref):
    features = part_ref.shape[1]
    got = jnp.concatenate([got0_ref[...], got1_ref[...]], axis=0)
    high, low = split(got)
    last = ef_ref[2 * features :, :]
    ends = dot_t(high, last) + dot_t(low, last)
    out_ref[...] = (part_ref[...] + seam_spread(spread_ref, ends)).astype(BF)


def unpack_kernel(core_ref, mine_ref, other_ref, gef_ref, ges_ref, gnf_ref, gns_ref):
    half = mine_ref.shape[1]
    low_core = core_ref[0] == 0
    begin = 0
    for ref in (gef_ref, ges_ref, gnf_ref, gns_ref):
        size = ref.shape[0]
        mine = mine_ref[begin : begin + size, :]
        other = other_ref[begin : begin + size, :]
        ref[:, :half] = jnp.where(low_core, mine, other)
        ref[:, half:] = jnp.where(low_core, other, mine)
        begin += size


def call(kernel, outs, args, scalars=0, scratch=(), flops=0, name=None):
    return pl.pallas_call(
        kernel,
        out_shape=[jax.ShapeDtypeStruct(shape, kind) for shape, kind in outs],
        in_specs=[
            pl.BlockSpec(memory_space=pltpu.SMEM if i < scalars else pltpu.VMEM)
            for i in range(len(args))
        ],
        out_specs=[pl.BlockSpec(memory_space=pltpu.VMEM) for _ in outs],
        scratch_shapes=[pltpu.VMEM(shape, F32) for shape in scratch],
        compiler_params=pltpu.CompilerParams(vmem_limit_bytes=24 * 2**20),
        cost_estimate=pl.CostEstimate(flops=flops, transcendentals=0, bytes_accessed=flops // 1000),
        name=name,
    )(*args)


def shift(block, distance):
    count = lax.axis_size(PATCH)
    return lax.ppermute(block, PATCH, [((i - distance) % count, i) for i in range(count)])


def group_size(axes):
    return lax.axis_size(axes)


def sum_kernel(pieces_ref, side0_ref, side1_ref, out_ref, pass0_ref, pass1_ref):
    count = pieces_ref.shape[0]
    copies = out_ref.shape[0]
    pass0_ref[...] = side0_ref[...]
    pass1_ref[...] = side1_ref[...]
    total = lax.fori_loop(
        1,
        count,
        lambda i, acc: acc + pieces_ref[i].astype(F32),
        pieces_ref[0].astype(F32),
        unroll=7,
    ).astype(BF)

    def store(i, carry):
        out_ref[i] = total
        return carry

    lax.fori_loop(0, copies, store, 0, unroll=8)


def sum_and_copy(pieces, side0, side1, copies, name):
    return call(
        sum_kernel,
        [
            ((copies,) + pieces.shape[1:], BF),
            (side0.shape, side0.dtype),
            (side1.shape, side1.dtype),
        ],
        (pieces, side0, side1),
        flops=pieces.size,
        name=name,
    )


def add_kernel(pieces_ref, out_ref):
    out_ref[...] = (pieces_ref[0].astype(F32) + pieces_ref[1].astype(F32)).astype(BF)


def swap_cores(block):
    count = lax.axis_size("c")
    return lax.ppermute(block, "c", [((i + 1) % count, i) for i in range(count)])


def sum_everywhere(pack, back0, back1):
    inner = group_size(INNER)
    outer = group_size(OUTER)
    rows, lanes = pack.shape[1:]
    (pair,) = call(
        add_kernel,
        [((rows, lanes), BF)],
        (lax.all_to_all(pack, "c", 0, 0),),
        flops=pack.size,
        name="core_sum",
    )
    pieces = lax.all_to_all(pair.reshape(inner, rows // inner, lanes), INNER, 0, 0)
    pieces, back0, back1 = sum_and_copy(pieces, back0, back1, outer, "inner_sum")
    pieces = lax.all_to_all(pieces, OUTER, 0, 0)
    got0 = shift(back0, 1)
    got1 = shift(back1, 2)
    pieces, got0, got1 = sum_and_copy(pieces, got0, got1, inner, "outer_sum")
    mine = lax.all_to_all(pieces, INNER, 0, 0).reshape(rows, lanes)
    return mine, swap_cores(mine), got0, got1


def local(
    nodes,
    edges,
    edge_ends,
    edge_count,
    send_rows,
    cotangent,
    edge_first,
    edge_second,
    node_first,
    node_second,
):
    node_rows = nodes[0]
    edge_rows = edges[0]
    cot = cotangent[0]
    verts, features = node_rows.shape
    slots = edge_rows.shape[0]
    hops, seam = send_rows.shape
    assert hops == 2
    ends = edge_ends.T
    core = lax.axis_index("c").astype(jnp.int32).reshape(1)
    seam16 = ((seam, features), BF)
    seam32 = ((seam, features), F32)
    unit = 2 * features * features

    out0, out1, node_rows, ends, edge_first, edge_rows, pick, spread = load(
        (send_rows, node_rows, ends, edge_first, edge_rows)
    )
    halo0 = shift(out0, -1)
    halo1 = shift(out1, -2)
    part, pairs, far = call(
        edge_local_kernel,
        [((slots, features), F32), ((slots, verts), BF), ((slots, hops * seam), BF)],
        (edge_count, ends, node_rows, edge_rows, edge_first),
        scalars=1,
        flops=7 * slots * unit,
        name="edge_local",
    )
    pre, hidden, normed, inv, new_edge, back0, back1 = call(
        functools.partial(edge_forward_kernel, verts),
        [
            ((slots, features), F32),
            ((slots, features), BF),
            ((slots, features), F32),
            ((slots, 1), F32),
            ((slots, features), BF),
            seam32,
            seam32,
        ],
        (edge_count, ends, halo0, halo1, edge_rows, part, far, edge_first, edge_second),
        scalars=1,
        scratch=[(hops * seam, features)],
        flops=4 * slots * unit,
        name="edge_forward",
    )
    got0 = shift(back0, 1)
    got1 = shift(back1, 2)
    tall = (verts, features)
    (agg,) = call(
        aggregate_kernel,
        [(tall, F32)],
        (edge_count, ends, new_edge),
        scalars=1,
        flops=4 * slots * unit,
        name="aggregate",
    )
    new_nodes, agg16, node_hidden, d_out, d_pre, d_agg, out0, out1 = call(
        node_kernel,
        [(tall, BF)] * 6 + [seam16, seam16],
        (pick, spread, node_rows, cot, agg, got0, got1, node_first, node_second),
        flops=8 * verts * unit,
        name="node",
    )
    d_halo0 = shift(out0, -1)
    d_halo1 = shift(out1, -2)
    node_grads, grad_part, up = call(
        fill_kernel,
        [((3 * features, features), BF), (tall, F32), ((slots, features), F32)],
        (node_rows, cot, agg16, node_hidden, d_out, d_pre, d_agg, node_first, pairs),
        flops=4 * slots * unit,
        name="fill",
    )
    grad_edges, pack, grad_part, back0, back1 = call(
        edge_backward_kernel,
        [
            ((slots, features), BF),
            ((2, 7 * features, features // 2), BF),
            (tall, F32),
            seam32,
            seam32,
        ],
        (
            edge_count,
            ends,
            node_rows,
            halo0,
            halo1,
            edge_rows,
            up,
            far,
            d_halo0,
            d_halo1,
            pre,
            hidden,
            normed,
            inv,
            edge_first,
            edge_second,
            node_grads,
            grad_part,
        ),
        scalars=1,
        scratch=[tall, tall, (hops * seam, features), (features, features), (features, features)],
        flops=12 * slots * unit,
        name="edge_backward",
    )
    mine, other, got0, got1 = sum_everywhere(pack, back0, back1)
    (grad_nodes,) = call(
        finish_kernel,
        [(tall, BF)],
        (spread, grad_part, got0, got1, edge_first),
        flops=verts * unit,
        name="finish",
    )
    grad_ef, grad_es, grad_nf, grad_ns = call(
        unpack_kernel,
        [
            ((3 * features, features), BF),
            ((features, features), BF),
            ((2 * features, features), BF),
            ((features, features), BF),
        ],
        (core, mine, other),
        scalars=1,
        flops=1000,
        name="unpack",
    )
    return (
        new_nodes[None],
        grad_nodes[None],
        grad_edges[None],
        grad_ef,
        grad_es,
        grad_nf,
        grad_ns,
    )


def solution(mesh):
    fine = Mesh(mesh.devices.reshape(PATCH_SPLIT + (mesh.shape["rep"],)), PATCH + ("rep",))
    placed = (
        P("rep", PATCH, None),
        P("rep", PATCH, None),
        P(PATCH, None),
        P(PATCH),
        P(PATCH, None),
        P("rep", PATCH, None),
        P(),
        P(),
        P(),
        P(),
    )
    return jax.shard_map(
        local,
        mesh=fine,
        in_specs=placed,
        out_specs=(
            P("rep", PATCH, None),
            P("rep", PATCH, None),
            P("rep", PATCH, None),
            P(),
            P(),
            P(),
            P(),
        ),
        check_vma=False,
    )
```
